32 devices in a mesh: rows: 8 (over z, y), chan: 4 (over x, core).
Axes of the slice: x: 2, y: 2, z: 4, core: 2. Of those that a mesh axis runs over, the one named last changes fastest.
Arguments:
- radiances: float32 [16, 16384], P('chan', 'rows'), may hold values from -6 to 6
- band: int32 [16384, 1], P('rows'), may hold values from 0 to 7; in each aligned block of 2048 rows (0 to 2047, 2048 to 4095, ...) at most 512 rows name the same one
- row_in_band: int32 [16384], P('rows'), may hold values from 0 to 3
- column: int32 [16384], P('rows'), may hold values from 0 to 1439
Outputs:
- cell_count: int32 [32, 1440], P('rows')
- cell_mean: float32 [16, 32, 1440], P('chan', 'rows')
- cell_var: float32 [16, 32, 1440], P('chan', 'rows')
- cell_spread: float32 [32, 1440], P('rows')
- departure: float32 [16, 16384], P('chan', 'rows')
The draws below stay inside these ranges and needn't reach their ends.
Inputs may be any that keep to these rules, and one draw needn't show every extreme that they name: Within each aligned block of 2048 observations (one scan-time shard) no band is named by more than 512 observations, and in some blocks one band is named by exactly 512.
All inputs are finite; a program needn't handle non-finite values.
Results may differ from the reference program's by a relative error of at most 0.0003.
Values sent between devices are 32-bit elements.
A program may use at most 64 MiB of HBM per device.

```python
import math
import jax
import jax.numpy as jnp
import numpy as np
from jax import lax

CHAN = 16
COLS = 1440
ROWS_DEV = 4
OBS_DEV = 2048
LATS = 32
OBS = 16384
CAP = 512
N_ROWS = 8


def touch_ends(result, key, smallest, high):
    index_at = [jax.random.randint(jax.random.fold_in(key, axis), (), 0, length) for axis, length in enumerate(result.shape)]
    longest = result.shape.index(max(result.shape))
    neighbour = index_at[:longest] + [(index_at[longest] + 1) % result.shape[longest]] + index_at[longest + 1:]
    return result.at[tuple(index_at)].set(smallest).at[tuple(neighbour)].set(high)


def shard_levels(rng, shape, cuts, smallest, top_value):
    def one(dim, parts):
        draws = jax.random.uniform(jax.random.fold_in(jax.random.fold_in(rng, 6), dim), (parts,), jnp.float32, smallest / len(cuts), top_value / len(cuts))
        return jnp.repeat(jnp.exp(draws), shape[dim] // parts).reshape((-1,) + (1,) * (len(shape) - dim - 1))

    level = one(*cuts[0])
    for cut in cuts[1:]:
        level = level * one(*cut)
    return level


def shared_out(key, own, number, rows, number_of, top, reach, lean):
    sequence = jax.random.permutation(key, number_of)
    crowded, ordinary = portions_of(number_of, rows * top, reach, lean, True), portions_of(number_of, rows * top, reach, lean, False)
    places = jnp.arange(number_of)

    def named(sizes, turn):
        used = int((sizes > 0).sum())
        fixed = max(1, used // 4)
        passed = fixed + (places - fixed + turn * (used - fixed)) % max(1, number_of - fixed)
        return jnp.zeros((number_of,), jnp.int32).at[sequence[jnp.where(places < fixed, places, passed)]].set(jnp.asarray(sizes, jnp.int32))

    sizes = jnp.where(number % 4 == 0, named(crowded, number // 4), named(ordinary, number - number // 4 - 1))
    mixed = jax.random.permutation(jax.random.fold_in(own, 3), number_of)
    source_of, sink = mixed[0:number_of // 2 * 2:2], mixed[1:number_of // 2 * 2:2]
    margin = jnp.minimum(sizes[source_of] - 1, reach - sizes[sink]) // 2
    margin = jnp.where((source_of == sequence[0]) | (sink == sequence[0]) | (sizes[sink] == 0), 0, jnp.maximum(margin, 0))
    passed = jax.random.randint(jax.random.fold_in(own, 4), (number_of // 2,), 0, 1 << 20) % (margin + 1)
    sizes = sizes.at[source_of].add(-passed).at[sink].add(passed)
    labels = jnp.searchsorted(jnp.cumsum(sizes), jnp.arange(rows * top), side="right").astype(jnp.int32)
    grid = labels.reshape(top, rows).T
    grid = grid[jax.random.permutation(jax.random.fold_in(own, 1), rows)]
    turn = jax.random.randint(jax.random.fold_in(own, 2), (rows, 1), 0, top)
    return jnp.take_along_axis(grid, (jnp.arange(top)[None, :] + turn) % top, axis=1)


def portions_of(count, total, limit, lean, full):
    weights = [(1 << 20) // math.isqrt(rank ** lean) + 1 for rank in range(1, count + 1)]
    largest = limit if full else min(limit, max(-(-total // count), total * weights[0] // sum(weights)))
    least = 1 if total - largest >= count - 1 else 0
    counts, surplus = [largest] + [least] * (count - 1), total - largest - least * (count - 1)
    while surplus > 0:
        free = [i for i in range(1, count) if counts[i] < largest] or [i for i in range(1, count) if counts[i] < limit]
        pool, budget = sum([weights[i] for i in free]), surplus
        for i in free:
            addition = min(limit - counts[i], max(1, budget * weights[i] // pool), surplus)
            counts[i] = counts[i] + addition
            surplus = surplus - addition
    return np.array(counts)


def noise(own_key, extent, deviation, most, shards=(), held_as=jnp.bfloat16):
    level = shard_levels(own_key, extent, shards, -0.22, 0.18) if shards else 1.0
    values = jax.random.normal(own_key, extent, jnp.float32) * deviation * level
    return jnp.minimum(jnp.maximum(values, -most), most).astype(held_as)


def setup_inputs(seed: int = 0) -> dict:
    arg_keys = jax.random.split(jax.random.key(seed), 5)
    radiances = noise(arg_keys[0], (CHAN, OBS), 1.0, 6.0, ((0, 4), (1, 8)), jnp.float32)
    band_keys = jax.random.split(jax.random.fold_in(arg_keys[1], 1), OBS // OBS_DEV)
    band_turns = jax.random.permutation(jax.random.fold_in(arg_keys[1], 3), OBS // OBS_DEV)
    band = jax.vmap(lambda own, number: shared_out(jax.random.fold_in(arg_keys[1], 2), own, number, OBS_DEV, N_ROWS, 1, CAP, 2))(band_keys, band_turns).reshape((OBS, 1))
    row_in_band = touch_ends(jax.random.randint(arg_keys[2], (OBS,), 0, ROWS_DEV), jax.random.fold_in(arg_keys[2], 1), 0, ROWS_DEV - 1).astype(jnp.int32)
    column = touch_ends(jax.random.randint(arg_keys[3], (OBS,), 0, COLS), jax.random.fold_in(arg_keys[3], 1), 0, COLS - 1).astype(jnp.int32)
    return {"radiances": radiances, "band": band, "row_in_band": row_in_band, "column": column}


def reference(radiances, band, row_in_band, column):
    lat = band[:, 0] * ROWS_DEV + row_in_band
    cell = (lat * COLS + column).astype(jnp.int32)
    cells = LATS * COLS
    ones = jnp.ones(cell.shape, jnp.float32)
    count = jax.ops.segment_sum(ones, cell, num_segments=cells)
    values = radiances.astype(jnp.float32).T
    first = jax.ops.segment_sum(values, cell, num_segments=cells)
    second = jax.ops.segment_sum(values * values, cell, num_segments=cells)
    denom = jnp.maximum(count, 1.0)[:, None]
    mean = first / denom
    var = jnp.maximum(second / denom - mean * mean, 0.0)
    spread = lax.optimization_barrier(jnp.sum(var, axis=1))
    scale = lax.rsqrt(1.0 + spread / CHAN)
    departure = (radiances - mean[cell].T) * scale[cell][None, :]
    cell_count = count.reshape(LATS, COLS).astype(jnp.int32)
    cell_mean = mean.T.reshape(CHAN, LATS, COLS)
    cell_var = var.T.reshape(CHAN, LATS, COLS)
    return (cell_count, cell_mean, cell_var, spread.reshape(LATS, COLS), departure)
```

```python
import functools

import jax
import jax.numpy as jnp
from jax import lax
from jax.experimental import pallas as pl
from jax.experimental.pallas import tpu as pltpu
from jax.sharding import PartitionSpec as P

CHAN = 16
COLS = 1440
ROWS_DEV = 4
LOW = 256
LANES = 128
BLOCKS = -(-COLS // LOW)
QS = BLOCKS * ROWS_DEV
F32 = jnp.float32
BF16 = jnp.bfloat16
MESH = pl.DeviceIdType.MESH
NT = (((1,), (1,)), ((), ()))
NN = (((1,), (0,)), ((), ()))


def iota(shape, axis):
    return lax.broadcasted_iota(jnp.int32, shape, axis)


def onehot(mask):
    return jnp.where(mask, 1.0, 0.0)


def two(values):
    high = values.astype(BF16).astype(F32)
    return high, values - high


def dot(a, b, dims):
    return lax.dot_general(a, b, dims, preferred_element_type=F32)


def flip(index, bits):
    out, bit = index, 1
    while bit <= bits:
        if bits & bit:
            out = out + bit - 2 * bit * ((index // bit) % 2)
        bit *= 2
    return out


def rank_of(dest, nrows):
    obs = dest.shape[1]
    nblock = obs // 128
    hot = onehot(iota((nrows, obs), 0) == dest)
    stacked = jnp.concatenate([hot[:, b * 128 : (b + 1) * 128] for b in range(nblock)], axis=0)
    stacked_b = stacked.astype(BF16)
    size = nblock * nrows
    upper = onehot(iota((128, 128), 0) <= iota((128, 128), 1)).astype(BF16)
    inner = dot(stacked_b, upper, NN)
    r, c = iota((size, size), 0), iota((size, size), 1)
    earlier = onehot((c < r) & (lax.rem(r - c + size, nrows) == 0)).astype(BF16)
    before = jnp.sum(dot(earlier, stacked_b, NN), axis=1, keepdims=True)
    ranks = stacked * (inner + before)
    rows = [
        jnp.sum(ranks[b * nrows : (b + 1) * nrows], axis=0, keepdims=True) for b in range(nblock)
    ]
    return (jnp.concatenate(rows, axis=1) - 1.0).astype(jnp.int32)


def spill(out, values):
    for j in range(BLOCKS):
        start = j * LOW
        width = min(LOW, COLS - start)
        out[:, start : start + width] = values[j * ROWS_DEV : (j + 1) * ROWS_DEV, :width].astype(
            out.dtype
        )


def folded(row):
    lines = row.shape[1] // LANES
    return jnp.concatenate([row[:, k * LANES : (k + 1) * LANES] for k in range(lines)], axis=0)


def take(row, lane):
    return jnp.take_along_axis(
        jnp.broadcast_to(row, lane.shape), lane, axis=1, mode="promise_in_bounds"
    )


def look(grids, cells):
    tile, lane = cells // LANES - LOW // LANES, cells & (LANES - 1)
    found = [jnp.zeros(cells.shape, F32) for _ in grids]
    for q in range(QS):
        for half in range(LOW // LANES):
            here = tile == q * (LOW // LANES) + half
            span = slice(half * LANES, (half + 1) * LANES)
            for g, grid in enumerate(grids):
                found[g] = jnp.where(here, take(grid[q : q + 1, span], lane), found[g])
    return found


def sums_of(arrived, slots):
    fields, lines = arrived.shape[1] - 1, arrived.shape[2]
    left, right = [], []
    for d in slots:
        cells = arrived[d, fields].astype(jnp.int32)
        low, high = cells & (LOW - 1), cells // LOW - 1
        features = []
        for f in range(fields):
            x = arrived[d, f]
            features.append(two(x) + two(x * x))
        for t in range(lines):
            right.append(onehot(iota((LOW, LANES), 0) == low[t : t + 1]).astype(BF16))
            quads = onehot(iota((QS, LANES), 0) == high[t : t + 1])
            rows = [quads]
            for k in range(4):
                rows += [quads * features[f][k][t : t + 1] for f in range(fields)]
            left.append(jnp.concatenate(rows, axis=0).astype(BF16))
    return dot(jnp.concatenate(left, axis=1), jnp.concatenate(right, axis=1), NT)


def kernel(
    nrows,
    nchan,
    rad_in,
    band_in,
    rib_in,
    col_in,
    cnt_out,
    mean_out,
    var_out,
    spr_out,
    dep_out,
    rad_ref,
    band_ref,
    rib_ref,
    col_ref,
    rank_hot,
    staged,
    sent,
    arrived,
    grid,
    part_s,
    part_r,
    pair,
    pairs,
    back_s,
    back_r,
    scale_s,
    scale_r,
    turned,
    ready,
    ins,
    so,
    ro,
    sp,
    rp,
    sg,
    rg,
    sb,
    rb,
    ss,
    rs,
):
    me = lax.axis_index("rows")
    mc = lax.axis_index("chan")
    fields, obs = rad_ref.shape
    cap = rank_hot.shape[0]
    lines = cap // LANES
    npair = nchan // 2
    far = list(range(nrows - 1, 0, -1))
    row_peer = [flip(me, d) for d in range(nrows)]
    chan_peer = [lax.rem(mc + 2 * j, nchan) for j in range(npair)]
    partner = flip(mc, 1)

    def remote(src, dst, send, recv, **to):
        return pltpu.make_async_remote_copy(
            src_ref=src,
            dst_ref=dst,
            send_sem=send,
            recv_sem=recv,
            device_id=to,
            device_id_type=MESH,
        )

    barrier = pltpu.get_barrier_semaphore()
    for d in far:
        pl.semaphore_signal(
            barrier, inc=1, device_id={"rows": row_peer[d]}, device_id_type=MESH
        )
    for peer in chan_peer[1:] + [partner]:
        pl.semaphore_signal(barrier, inc=1, device_id={"chan": peer}, device_id_type=MESH)
    fetches = [
        pltpu.make_async_copy(a, b, ins.at[i])
        for i, (a, b) in enumerate(
            ((band_in, band_ref), (rad_in, rad_ref), (rib_in, rib_ref), (col_in, col_ref))
        )
    ]
    for fetch in fetches:
        fetch.start()

    fetches[0].wait()
    dest = band_ref[...]
    rank = rank_of(dest, nrows)
    rank_hot[...] = onehot(iota((cap, obs), 0) == rank).astype(BF16)
    for fetch in fetches[1:]:
        fetch.wait()
    high, rest = two(rad_ref[...])
    middle, low = two(rest)
    col = col_ref[...]
    code = (col // LOW) * ROWS_DEV + rib_ref[...] + 1
    tail = jnp.zeros((8 - fields - 1, obs), F32)
    none = jnp.zeros((1, obs), F32)
    group = 24
    payload = jnp.concatenate(
        [high, (code * LOW).astype(F32), tail]
        + [middle, (col & (LOW - 1)).astype(F32), tail]
        + [low, none, tail],
        axis=0,
    )
    left = jnp.concatenate(
        [jnp.where(dest == row_peer[d], payload, 0.0) for d in range(nrows)], axis=0
    ).astype(BF16)
    placed = dot(left, rank_hot[...], NT)
    for d in range(nrows):
        part = placed[d * group : (d + 1) * group]
        values = (part[0:8] + part[8:16]) + part[16:24]
        for t in range(lines):
            at = (d * lines + t) * 8
            staged[at : at + 8] = values[:, t * LANES : (t + 1) * LANES]
    for d in far + [0]:
        target = sent if d > 0 else arrived
        for f in range(fields + 1):
            target[d, f] = staged[pl.ds(d * lines * 8 + f, lines, stride=8), :]

    pl.semaphore_wait(barrier, nrows - 1 + npair)
    out_copies = {}
    for d in far:
        out_copies[d] = remote(
            sent.at[d], arrived.at[d], so.at[d], ro.at[d], rows=row_peer[d]
        )
        out_copies[d].start()
    for j in range(1, npair):
        pl.semaphore_signal(ready, inc=1, device_id={"chan": chan_peer[j]}, device_id_type=MESH)

    half = nrows // 2
    groups = [[0], list(range(1, half)), list(range(half, nrows))]
    total = None
    for slots in groups:
        for d in slots:
            if d > 0:
                out_copies[d].wait_recv()
        sums = sums_of(arrived, slots)
        total = sums if total is None else total + sums

    def feature(k, f):
        at = (1 + k * fields + f) * QS
        return total[at : at + QS]

    count = total[0:QS]
    inverse = 1.0 / jnp.maximum(count, 1.0)
    partial = None
    means, variances = [], []
    for f in range(fields):
        mean = (feature(0, f) + feature(1, f)) * inverse
        second = (feature(2, f) + feature(3, f)) * inverse
        variance = jnp.maximum(second - mean * mean, 0.0)
        means.append(mean)
        variances.append(variance)
        partial = variance if partial is None else partial + variance
    part_s[...] = partial
    part_copy = remote(part_s, part_r, sp.at[0], rp.at[0], chan=partner)
    part_copy.start()
    for f in range(fields):
        grid[f] = means[f]

    order = far + [0]
    per = max(1, 8 // lines)
    bundles = [order[i : i + per] for i in range(0, nrows, per)]
    cells_of = []
    back_copies = {}
    for slots in bundles:

        def stack(f):
            return jnp.concatenate([arrived[d, f] for d in slots], axis=0)

        cells = stack(fields).astype(jnp.int32)
        cells_of.append(cells)
        found = look([grid.at[f] for f in range(fields)], cells)
        for f in range(fields):
            diff = stack(f) - found[f]
            for i, d in enumerate(slots):
                target = back_s if d > 0 else back_r
                target[d, f] = diff[i * lines : (i + 1) * lines]
        for d in slots:
            if d > 0:
                back_copies[d] = remote(
                    back_s.at[d], back_r.at[d], sb.at[d], rb.at[d], rows=row_peer[d]
                )
                back_copies[d].start()

    part_copy.wait_recv()
    both = part_s[...] + part_r[...]
    pair[...] = both
    mine = mc // 2
    pairs[mine] = both
    pl.semaphore_wait(ready, npair - 1)
    scale_copies = []
    for slots, cells in zip(bundles, cells_of):
        found = look([pair], cells)[0]
        for i, d in enumerate(slots):
            scale_s[d] = found[i * lines : (i + 1) * lines]
            if d == 0:
                scale_r[0] = found[i * lines : (i + 1) * lines]
        for d in slots:
            for j in list(range(1, npair)) + [0]:
                if d + j == 0:
                    continue
                slot = j * nrows + d
                copy = remote(
                    scale_s.at[d],
                    scale_r.at[slot],
                    ss.at[slot],
                    rs.at[slot],
                    rows=row_peer[d],
                    chan=chan_peer[j],
                )
                copy.start()
                scale_copies.append((d, copy))
    pair_copies = []
    for j in range(1, npair):
        copy = remote(pairs.at[mine], pairs.at[mine], sg.at[j], rg.at[j], chan=chan_peer[j])
        copy.start()
        pair_copies.append(copy)

    spill(cnt_out, count)
    for f in range(fields):
        spill(mean_out.at[f], means[f])
        spill(var_out.at[f], variances[f])

    rank = folded(rank)
    place = jnp.bitwise_xor(folded(dest), me) * lines + rank // LANES
    lane = rank & (LANES - 1)
    found = [jnp.zeros(rank.shape, F32) for _ in range(fields + 1)]
    back_order = [0] + list(range(1, half)) + list(range(nrows - 1, half - 1, -1))
    for d in back_order:
        if d > 0:
            back_copies[d].wait_recv()
        for t in range(lines):
            here = place == d * lines + t
            for f in range(fields):
                found[f] = jnp.where(here, take(back_r[d, f, t : t + 1], lane), found[f])
    for copy in pair_copies:
        copy.wait_recv()
    spread = pairs[0]
    for p in range(1, npair):
        spread = spread + pairs[p]
    spill(spr_out, spread)
    for d in back_order:
        for to, copy in scale_copies:
            if to == d:
                copy.wait_recv()
        for t in range(lines):
            here = place == d * lines + t
            row = scale_r[d, t : t + 1]
            for j in range(1, npair):
                row = row + scale_r[j * nrows + d, t : t + 1]
            found[fields] = jnp.where(here, take(row, lane), found[fields])
    scale = lax.rsqrt(1.0 + found[fields] / CHAN)
    many = obs // LANES
    for f in range(fields):
        turned[f * many : (f + 1) * many] = found[f] * scale
    for k in range(many):
        dep_out[:, k * LANES : (k + 1) * LANES] = turned[pl.ds(k, fields, stride=many), :]

    for copy in list(out_copies.values()) + list(back_copies.values()):
        copy.wait_send()
    for copy in [part_copy] + pair_copies + [copy for _, copy in scale_copies]:
        copy.wait_send()


def finish(*refs):
    half = (len(refs) - 1) // 2
    sems = refs[-1]
    copies = [
        pltpu.make_async_copy(a, b, sems.at[i])
        for i, (a, b) in enumerate(zip(refs[:half], refs[half : 2 * half]))
    ]
    for copy in copies:
        copy.start()
    for copy in copies:
        copy.wait()


def body(radiances, band, row_in_band, column):
    nrows = lax.axis_size("rows")
    nchan = lax.axis_size("chan")
    fields, obs = radiances.shape
    cap = 2 * obs // nrows
    lines = cap // LANES
    npair = nchan // 2
    vmem = pl.BlockSpec(memory_space=pltpu.VMEM)
    anywhere = pl.BlockSpec(memory_space=pl.ANY)
    dma = pltpu.SemaphoreType.DMA
    shapes = (
        ((ROWS_DEV, COLS), jnp.int32),
        ((fields, ROWS_DEV, COLS), F32),
        ((fields, ROWS_DEV, COLS), F32),
        ((ROWS_DEV, COLS), F32),
        ((fields, obs), F32),
    )
    held = pl.pallas_call(
        functools.partial(kernel, nrows, nchan),
        out_shape=tuple(pltpu.VMEM(s, t) for s, t in shapes),
        in_specs=[pl.BlockSpec(memory_space=pltpu.HBM)] * 4,
        out_specs=(vmem,) * len(shapes),
        scratch_shapes=[
            pltpu.VMEM((fields, obs), F32),
            pltpu.VMEM((1, obs), jnp.int32),
            pltpu.VMEM((1, obs), jnp.int32),
            pltpu.VMEM((1, obs), jnp.int32),
            pltpu.VMEM((cap, obs), BF16),
            pltpu.VMEM((nrows * lines * 8, LANES), F32),
            pltpu.VMEM((nrows, fields + 1, lines, LANES), F32),
            pltpu.VMEM((nrows, fields + 1, lines, LANES), F32),
            pltpu.VMEM((fields, QS, LOW), F32),
            pltpu.VMEM((QS, LOW), F32),
            pltpu.VMEM((QS, LOW), F32),
            pltpu.VMEM((QS, LOW), F32),
            pltpu.VMEM((npair, QS, LOW), F32),
            pltpu.VMEM((nrows, fields, lines, LANES), F32),
            pltpu.VMEM((nrows, fields, lines, LANES), F32),
            pltpu.VMEM((nrows, lines, LANES), F32),
            pltpu.VMEM((npair * nrows, lines, LANES), F32),
            pltpu.VMEM((fields * obs // LANES, LANES), F32),
            pltpu.SemaphoreType.REGULAR,
            dma((4,)),
            dma((nrows,)),
            dma((nrows,)),
            dma((1,)),
            dma((1,)),
            dma((npair,)),
            dma((npair,)),
            dma((nrows,)),
            dma((nrows,)),
            dma((npair * nrows,)),
            dma((npair * nrows,)),
        ],
        compiler_params=pltpu.CompilerParams(
            collective_id=0, has_side_effects=True, vmem_limit_bytes=32 * 1024 * 1024
        ),
    )(
        *(
            pltpu.with_memory_space_constraint(x, pltpu.HBM)
            for x in (
                radiances,
                band.reshape(1, obs),
                row_in_band.reshape(1, obs),
                column.reshape(1, obs),
            )
        )
    )
    return pl.pallas_call(
        finish,
        out_shape=tuple(jax.ShapeDtypeStruct(s, t) for s, t in shapes),
        in_specs=[vmem] * len(shapes),
        out_specs=(anywhere,) * len(shapes),
        scratch_shapes=[dma((len(shapes),))],
        compiler_params=pltpu.CompilerParams(vmem_limit_bytes=32 * 1024 * 1024),
    )(*held)


def solution(mesh):
    in_specs = (P("chan", "rows"), P("rows", None), P("rows"), P("rows"))
    out_specs = (
        P("rows", None),
        P("chan", "rows", None),
        P("chan", "rows", None),
        P("rows", None),
        P("chan", "rows"),
    )
    return jax.shard_map(body, mesh=mesh, in_specs=in_specs, out_specs=out_specs, check_vma=False)
```

```python
import functools

import jax
import jax.numpy as jnp
from jax import lax
from jax.experimental import pallas as pl
from jax.experimental.pallas import tpu as pltpu
from jax.sharding import PartitionSpec as P

CHAN = 16
PACK = 16
COLS = 1440
ROWS_DEV = 4
LOW = 256
LANES = 128
BLOCKS = -(-COLS // LOW)
QS = BLOCKS * ROWS_DEV
F32 = jnp.float32
BF16 = jnp.bfloat16
MESH = pl.DeviceIdType.MESH
NT = (((1,), (1,)), ((), ()))
NN = (((1,), (0,)), ((), ()))


def iota(shape, axis):
    return lax.broadcasted_iota(jnp.int32, shape, axis)


def onehot(mask):
    return jnp.where(mask, 1.0, 0.0)


def two(values):
    high = values.astype(BF16).astype(F32)
    return high, values - high


def product(accs, tiles, transpose):
    for i in range(0, len(tiles), 2):
        pair = tiles[i : i + 2]
        if len(pair) < 2:
            pair.append([jnp.zeros_like(x) for x in pair[0]])
        left, right = (jnp.concatenate(x, axis=1) for x in zip(*pair))
        unit, register = i // 2 % 2, i // 4 % 2
        pltpu.matmul_push_rhs(
            right, staging_register=register, mxu_index=unit, transpose=transpose
        )
        pltpu.matmul_acc_lhs(accs[unit], left, load_staged_rhs=register)


def flip(index, bits):
    out, bit = index, 1
    while bit <= bits:
        if bits & bit:
            out = out + bit - 2 * bit * ((index // bit) % 2)
        bit *= 2
    return out


def rank_of(dest, nrows, acc):
    obs = dest.shape[1]
    nblock = obs // LOW
    hot = [
        onehot(iota((nrows, LOW), 0) == dest[:, b * LOW : (b + 1) * LOW]) for b in range(nblock)
    ]
    upper = onehot(iota((LOW, LOW), 0) < iota((LOW, LOW), 1)).astype(BF16)
    pltpu.matmul_push_rhs(upper, staging_register=0, mxu_index=0)
    pltpu.matmul_acc_lhs(acc, jnp.concatenate(hot, axis=0).astype(BF16), load_staged_rhs=0)
    inner = pltpu.matmul_pop(acc)
    rows, before = [], None
    for b in range(nblock):
        count = inner[b * nrows : (b + 1) * nrows]
        if before is not None:
            count = count + before
        row = jnp.sum(hot[b] * count, axis=0, keepdims=True)
        rows += [row[:, k : k + LANES] for k in range(0, LOW, LANES)]
        size = jnp.sum(hot[b], axis=1, keepdims=True)
        before = size if before is None else before + size
    return rows


def spill(out, values):
    for j in range(BLOCKS):
        start = j * LOW
        width = min(LOW, COLS - start)
        out[:, start : start + width] = values[j * ROWS_DEV : (j + 1) * ROWS_DEV, :width].astype(
            out.dtype
        )


def folded(row):
    lines = row.shape[1] // LANES
    return jnp.concatenate([row[:, k * LANES : (k + 1) * LANES] for k in range(lines)], axis=0)


def take(row, lane):
    return jnp.take_along_axis(
        jnp.broadcast_to(row, lane.shape), lane, axis=1, mode="promise_in_bounds"
    )


def packed(row):
    return jnp.broadcast_to(row, (PACK, row.shape[1])).astype(BF16)


def steps(first, period=PACK):
    return (iota((PACK, LANES), 0) % period + first).astype(F32).astype(BF16)


def low_hot(row, size):
    wide = packed(row)
    one, zero = jnp.ones((PACK, LANES), BF16), jnp.zeros((PACK, LANES), BF16)
    return jnp.concatenate(
        [jnp.where(steps(b) == wide, one, zero) for b in range(0, size, PACK)], axis=0
    )


def tiles_of(arrived, col_hot, slots):
    fields, lines = arrived.shape[1] - 1, arrived.shape[2]
    one, zero = jnp.ones((PACK, LANES), BF16), jnp.zeros((PACK, LANES), BF16)
    tiles = []
    for d in slots:
        cells = arrived[d, fields]
        high = jnp.floor(cells * (1.0 / LOW))
        low, high = cells - high * LOW, high - 1.0
        features = []
        for f in range(fields):
            x = arrived[d, f]
            features += [two(x), two(x * x)]
        for t in range(lines):
            hot = low_hot(low[t : t + 1], LOW)
            col_hot[d, :, t * LANES : (t + 1) * LANES] = hot
            quad = packed(high[t : t + 1])
            pairs = [
                jnp.concatenate(
                    [jnp.broadcast_to(x[t : t + 1], (8, LANES)) for x in feature], axis=0
                ).astype(BF16)
                for feature in features
            ]
            rows = []
            for j in range(0, QS, 8):
                here = steps(j, 8) == quad
                rows += [jnp.where(here, x, zero) for x in pairs]
            for j in range(0, QS, PACK):
                rows.append(jnp.where(steps(j) == quad, one, zero))
            tiles.append([jnp.concatenate(rows, axis=0), hot])
    return tiles


def grids_of(total, fields):
    out = []
    for p in range(2 * fields):
        rows = []
        for j in range(QS // 8):
            at = (j * 2 * fields + p) * 16
            rows.append(total[at : at + 8] + total[at + 8 : at + 16])
        out.append(jnp.concatenate(rows, axis=0))
    at = QS // 8 * 2 * fields * 16
    return total[at : at + QS], out[0::2], out[1::2]


def kernel(
    nrows,
    nchan,
    rad_in,
    band_in,
    rib_in,
    col_in,
    cnt_out,
    mean_out,
    var_out,
    spr_out,
    dep_out,
    rad_ref,
    band_ref,
    rib_ref,
    col_ref,
    staged,
    sent,
    arrived,
    col_hot,
    part_s,
    part_r,
    pairs,
    share_s,
    share_r,
    back_s,
    back_r,
    scale_s,
    scale_r,
    turned,
    ready,
    ins,
    so,
    ro,
    sp,
    rp,
    sh,
    rh,
    sg,
    rg,
    sb,
    rb,
    ss,
    rs,
):
    me = lax.axis_index("rows")
    mc = lax.axis_index("chan")
    fields, obs = rad_ref.shape
    cap = 2 * obs // nrows
    lines = cap // LANES
    npair = nchan // 2
    far = list(range(nrows - 1, 0, -1))
    row_peer = [flip(me, d) for d in range(nrows)]
    chan_peer = [lax.rem(mc + 2 * j, nchan) for j in range(npair)]
    partner = flip(mc, 1)

    def remote(src, dst, send, recv, **to):
        return pltpu.make_async_remote_copy(
            src_ref=src,
            dst_ref=dst,
            send_sem=send,
            recv_sem=recv,
            device_id=to,
            device_id_type=MESH,
        )

    barrier = pltpu.get_barrier_semaphore()
    for d in far:
        pl.semaphore_signal(
            barrier, inc=1, device_id={"rows": row_peer[d]}, device_id_type=MESH
        )
    for peer in chan_peer[1:] + [partner]:
        pl.semaphore_signal(barrier, inc=1, device_id={"chan": peer}, device_id_type=MESH)
    fetches = [
        pltpu.make_async_copy(a, b, ins.at[i])
        for i, (a, b) in enumerate(
            ((band_in, band_ref), (rad_in, rad_ref), (rib_in, rib_ref), (col_in, col_ref))
        )
    ]
    for fetch in fetches:
        fetch.start()

    fetches[0].wait()
    dest = band_ref[...]

    def place_all(acc_rank, *accs):
        ranks = rank_of(dest, nrows, acc_rank)
        rank = folded(jnp.concatenate(ranks, axis=1)).astype(jnp.int32)
        wide = min(cap, LOW)
        parts = cap // wide
        hots, keys = [], []
        for k in range(obs // LANES):
            upper = jnp.floor(ranks[k] * (1.0 / wide))
            hots.append(low_hot(ranks[k] - upper * wide, LOW))
            names = jnp.bitwise_xor(dest[:, k * LANES : (k + 1) * LANES], me)
            keys.append(packed(names.astype(F32) * parts + upper))
        for fetch in fetches[1:]:
            fetch.wait()
        high, rest = two(rad_ref[...])
        middle, low = two(rest)
        col = col_ref[...]
        code = (col // LOW) * ROWS_DEV + rib_ref[...] + 1
        payload = jnp.concatenate(
            [high, middle, low]
            + [code.astype(F32), (col & (LOW - 1)).astype(F32)]
            + [jnp.zeros((PACK - 3 * fields - 2, obs), F32)],
            axis=0,
        ).astype(BF16)
        zero = jnp.zeros((PACK, LANES), BF16)
        left = []
        for k in range(obs // LANES):
            load = payload[:, k * LANES : (k + 1) * LANES]
            left.append(
                jnp.concatenate(
                    [
                        jnp.where(keys[k] == jnp.full((PACK, LANES), key, BF16), load, zero)
                        for key in range(nrows * parts)
                    ],
                    axis=0,
                )
            )
        product(accs, [list(x) for x in zip(left, hots)], True)
        placed = pltpu.matmul_pop(accs[0]) + pltpu.matmul_pop(accs[1])
        for d in far + [0]:
            target = sent if d > 0 else arrived
            for p in range(parts):
                part = placed[(d * parts + p) * PACK : (d * parts + p + 1) * PACK]
                values = (part[:fields] + part[fields : 2 * fields]) + part[2 * fields : 3 * fields]
                cells = part[3 * fields : 3 * fields + 1] * LOW + part[3 * fields + 1 : 3 * fields + 2]
                for i in range(wide // LANES):
                    t = p * (wide // LANES) + i
                    span = slice(i * LANES, (i + 1) * LANES)
                    at = (d * lines + t) * 8
                    staged[at : at + fields] = values[:, span]
                    staged[at + fields : at + fields + 1] = cells[:, span]
            for f in range(fields + 1):
                target[d, f] = staged[pl.ds(d * lines * 8 + f, lines, stride=8), :]
        return rank

    rows_placed = nrows * max(1, cap // LOW) * PACK
    rank = pl.run_scoped(
        place_all,
        pltpu.ACC(0)((nrows * obs // LOW, LOW), F32),
        pltpu.ACC(0)((rows_placed, LOW), F32),
        pltpu.ACC(1)((rows_placed, LOW), F32),
    )
    pl.semaphore_wait(barrier, nrows - 1 + npair)
    out_copies = {}
    for d in far:
        out_copies[d] = remote(
            sent.at[d], arrived.at[d], so.at[d], ro.at[d], rows=row_peer[d]
        )
        out_copies[d].start()
    for j in range(1, npair):
        pl.semaphore_signal(ready, inc=1, device_id={"chan": chan_peer[j]}, device_id_type=MESH)

    half_rows = nrows // 2
    back_copies, share_copies = {}, {}

    def cells_all(acc_0, acc_1, *looks):
        accs = (acc_0, acc_1)
        groups = [[0], list(range(1, half_rows)), list(range(half_rows, nrows))]
        for slots in groups:
            for d in slots:
                if d > 0:
                    out_copies[d].wait_recv()
            product(accs, tiles_of(arrived, col_hot, slots), True)

        total = pltpu.matmul_pop(accs[0]) + pltpu.matmul_pop(accs[1])
        count, firsts, seconds = grids_of(total, fields)
        inverse = 1.0 / jnp.maximum(count, 1.0)
        partial = None
        means, variances = [], []
        for f in range(fields):
            mean = firsts[f] * inverse
            variance = jnp.maximum(seconds[f] * inverse - mean * mean, 0.0)
            means.append(mean)
            variances.append(variance)
            partial = variance if partial is None else partial + variance

        split = [two(x) for x in means + [partial]]
        pad = jnp.zeros((-(fields + 1) * QS % PACK, LOW), F32)
        table = [jnp.concatenate([x[k] for x in split] + [pad], axis=0).astype(BF16) for k in (0, 1)]
        places = [(d, t) for d in far + [0] for t in range(lines)]
        for i in range(0, len(places), 2):
            unit, ring = i // 2 % 2, i // 4 % 2
            acc = looks[unit * 2 + ring]
            hot = jnp.concatenate(
                [col_hot[d, :, t * LANES : (t + 1) * LANES] for d, t in places[i : i + 2]], axis=1
            )
            pltpu.matmul_push_rhs(hot, staging_register=ring, mxu_index=unit)
            pltpu.matmul_acc_lhs(acc, table[0], load_staged_rhs=ring)
            pltpu.matmul_acc_lhs(acc, table[1])
            picked = pltpu.matmul_pop(acc)
            for k, (d, t) in enumerate(places[i : i + 2]):
                span = slice(k * LANES, (k + 1) * LANES)
                target = back_s if d > 0 else back_r
                high = arrived[d, fields, t : t + 1].astype(jnp.int32) // LOW - 1
                here = iota((QS, LANES), 0) == high
                for f in range(fields + 1):
                    both = picked[f * QS : (f + 1) * QS, span]
                    found = jnp.sum(jnp.where(here, both, 0.0), axis=0, keepdims=True)
                    if f < fields:
                        target[d, f, t : t + 1] = arrived[d, f, t : t + 1] - found
                    else:
                        share_s[d, t : t + 1] = found
                if t < lines - 1:
                    continue
                share_copies[d] = remote(
                    share_s.at[d], share_r.at[d], sh.at[d], rh.at[d], chan=partner
                )
                share_copies[d].start()
                if d > 0:
                    back_copies[d] = remote(
                        back_s.at[d], back_r.at[d], sb.at[d], rb.at[d], rows=row_peer[d]
                    )
                    back_copies[d].start()
        part_s[...] = partial
        part_copy = remote(part_s, part_r, sp.at[0], rp.at[0], chan=partner)
        part_copy.start()

        spill(cnt_out, count)
        for f in range(fields):
            spill(mean_out.at[f], means[f])
            spill(var_out.at[f], variances[f])
        pl.semaphore_wait(ready, npair - 1)
        scale_copies = []
        for d in far + [0]:
            share_copies[d].wait_recv()
            scale_s[d] = share_s[d] + share_r[d]
            if d == 0:
                scale_r[0] = share_s[d] + share_r[d]
            for j in list(range(1, npair)) + [0]:
                if d + j == 0:
                    continue
                slot = j * nrows + d
                copy = remote(
                    scale_s.at[d],
                    scale_r.at[slot],
                    ss.at[slot],
                    rs.at[slot],
                    rows=row_peer[d],
                    chan=chan_peer[j],
                )
                copy.start()
                scale_copies.append((d, copy))
        part_copy.wait_recv()
        mine = mc // 2
        pairs[mine] = part_s[...] + part_r[...]
        pair_copies = []
        for j in range(1, npair):
            copy = remote(pairs.at[mine], pairs.at[mine], sg.at[j], rg.at[j], chan=chan_peer[j])
            copy.start()
            pair_copies.append(copy)

        place = jnp.bitwise_xor(folded(dest), me) * lines + rank // LANES
        lane = rank & (LANES - 1)
        found = [jnp.zeros(rank.shape, F32) for _ in range(fields + 1)]
        far_half = list(range(nrows - 1, half_rows - 1, -1))
        returns = [list(range(half_rows)), far_half]
        for slots in returns:
            for d in slots:
                if d > 0:
                    back_copies[d].wait_recv()
            for d in slots:
                for t in range(lines):
                    here = place == d * lines + t
                    for f in range(fields):
                        found[f] = jnp.where(here, take(back_r[d, f, t : t + 1], lane), found[f])
        for slots in returns:
            for d, copy in scale_copies:
                if d in slots:
                    copy.wait_recv()
            for d in slots:
                for t in range(lines):
                    here = place == d * lines + t
                    row = scale_r[d, t : t + 1]
                    for j in range(1, npair):
                        row = row + scale_r[j * nrows + d, t : t + 1]
                    found[fields] = jnp.where(here, take(row, lane), found[fields])
        scale = lax.rsqrt(1.0 + found[fields] / CHAN)
        many = obs // LANES
        for f in range(fields):
            turned[f * many : (f + 1) * many] = found[f] * scale
        for k in range(many):
            dep_out[:, k * LANES : (k + 1) * LANES] = turned[pl.ds(k, fields, stride=many), :]
        for copy in pair_copies:
            copy.wait_recv()
        spread = pairs[0]
        for p in range(1, npair):
            spread = spread + pairs[p]
        spill(spr_out, spread)

        for copies in (out_copies, back_copies, share_copies):
            for copy in copies.values():
                copy.wait_send()
        for copy in [part_copy] + pair_copies + [copy for _, copy in scale_copies]:
            copy.wait_send()

    rows_summed = QS * 4 * fields + -(-QS // PACK) * PACK
    rows_looked = -(-(fields + 1) * QS // PACK) * PACK
    pl.run_scoped(
        cells_all,
        *(pltpu.ACC(unit)((rows_summed, LOW), F32) for unit in (0, 1)),
        *(pltpu.ACC(unit)((rows_looked, LOW), F32) for unit in (0, 0, 1, 1)),
    )


def finish(*refs):
    half = (len(refs) - 1) // 2
    sems = refs[-1]
    copies = [
        pltpu.make_async_copy(a, b, sems.at[i])
        for i, (a, b) in enumerate(zip(refs[:half], refs[half : 2 * half]))
    ]
    for copy in copies:
        copy.start()
    for copy in copies:
        copy.wait()


def body(radiances, band, row_in_band, column):
    nrows = lax.axis_size("rows")
    nchan = lax.axis_size("chan")
    fields, obs = radiances.shape
    cap = 2 * obs // nrows
    lines = cap // LANES
    npair = nchan // 2
    vmem = pl.BlockSpec(memory_space=pltpu.VMEM)
    anywhere = pl.BlockSpec(memory_space=pl.ANY)
    dma = pltpu.SemaphoreType.DMA
    shapes = (
        ((ROWS_DEV, COLS), jnp.int32),
        ((fields, ROWS_DEV, COLS), F32),
        ((fields, ROWS_DEV, COLS), F32),
        ((ROWS_DEV, COLS), F32),
        ((fields, obs), F32),
    )
    held = pl.pallas_call(
        functools.partial(kernel, nrows, nchan),
        out_shape=tuple(pltpu.VMEM(s, t) for s, t in shapes),
        in_specs=[pl.BlockSpec(memory_space=pltpu.HBM)] * 4,
        out_specs=(vmem,) * len(shapes),
        scratch_shapes=[
            pltpu.VMEM((fields, obs), F32),
            pltpu.VMEM((1, obs), jnp.int32),
            pltpu.VMEM((1, obs), jnp.int32),
            pltpu.VMEM((1, obs), jnp.int32),
            pltpu.VMEM((nrows * lines * 8, LANES), F32),
            pltpu.VMEM((nrows, fields + 1, lines, LANES), F32),
            pltpu.VMEM((nrows, fields + 1, lines, LANES), F32),
            pltpu.VMEM((nrows, LOW, cap), BF16),
            pltpu.VMEM((QS, LOW), F32),
            pltpu.VMEM((QS, LOW), F32),
            pltpu.VMEM((npair, QS, LOW), F32),
            pltpu.VMEM((nrows, lines, LANES), F32),
            pltpu.VMEM((nrows, lines, LANES), F32),
            pltpu.VMEM((nrows, fields, lines, LANES), F32),
            pltpu.VMEM((nrows, fields, lines, LANES), F32),
            pltpu.VMEM((nrows, lines, LANES), F32),
            pltpu.VMEM((npair * nrows, lines, LANES), F32),
            pltpu.VMEM((fields * obs // LANES, LANES), F32),
            pltpu.SemaphoreType.REGULAR,
            dma((4,)),
            dma((nrows,)),
            dma((nrows,)),
            dma((1,)),
            dma((1,)),
            dma((nrows,)),
            dma((nrows,)),
            dma((npair,)),
            dma((npair,)),
            dma((nrows,)),
            dma((nrows,)),
            dma((npair * nrows,)),
            dma((npair * nrows,)),
        ],
        compiler_params=pltpu.CompilerParams(
            collective_id=0, has_side_effects=True, vmem_limit_bytes=32 * 1024 * 1024
        ),
    )(
        *(
            pltpu.with_memory_space_constraint(x, pltpu.HBM)
            for x in (
                radiances,
                band.reshape(1, obs),
                row_in_band.reshape(1, obs),
                column.reshape(1, obs),
            )
        )
    )
    return pl.pallas_call(
        finish,
        out_shape=tuple(jax.ShapeDtypeStruct(s, t) for s, t in shapes),
        in_specs=[vmem] * len(shapes),
        out_specs=(anywhere,) * len(shapes),
        scratch_shapes=[dma((len(shapes),))],
        compiler_params=pltpu.CompilerParams(vmem_limit_bytes=32 * 1024 * 1024),
    )(*held)


def solution(mesh):
    in_specs = (P("chan", "rows"), P("rows", None), P("rows"), P("rows"))
    out_specs = (
        P("rows", None),
        P("chan", "rows", None),
        P("chan", "rows", None),
        P("rows", None),
        P("chan", "rows"),
    )
    return jax.shard_map(body, mesh=mesh, in_specs=in_specs, out_specs=out_specs, check_vma=False)
```

```python
import functools

import jax
import jax.numpy as jnp
from jax import lax
from jax.experimental import pallas as pl
from jax.experimental.pallas import tpu as pltpu
from jax.sharding import PartitionSpec as P

CHAN = 16
PACK = 16
COLS = 1440
ROWS_DEV = 4
LOW = 256
LANES = 128
BLOCKS = -(-COLS // LOW)
QS = BLOCKS * ROWS_DEV
F32 = jnp.float32
BF16 = jnp.bfloat16
MESH = pl.DeviceIdType.MESH
NT = (((1,), (1,)), ((), ()))
NN = (((1,), (0,)), ((), ()))


def iota(shape, axis):
    return lax.broadcasted_iota(jnp.int32, shape, axis)


def onehot(mask):
    return jnp.where(mask, 1.0, 0.0)


def two(values):
    high = values.astype(BF16).astype(F32)
    return high, values - high


def product(accs, tiles, transpose):
    for i in range(0, len(tiles), 2):
        pair = tiles[i : i + 2]
        if len(pair) < 2:
            pair.append([jnp.zeros_like(x) for x in pair[0]])
        left, right = (jnp.concatenate(x, axis=1) for x in zip(*pair))
        unit, register = i // 2 % 2, i // 4 % 2
        pltpu.matmul_push_rhs(
            right, staging_register=register, mxu_index=unit, transpose=transpose
        )
        pltpu.matmul_acc_lhs(accs[unit], left, load_staged_rhs=register)


def flip(index, bits):
    out, bit = index, 1
    while bit <= bits:
        if bits & bit:
            out = out + bit - 2 * bit * ((index // bit) % 2)
        bit *= 2
    return out


def rank_of(dest, nrows, acc):
    obs = dest.shape[1]
    nblock = obs // LOW
    hot = [
        onehot(iota((nrows, LOW), 0) == dest[:, b * LOW : (b + 1) * LOW]) for b in range(nblock)
    ]
    upper = onehot(iota((LOW, LOW), 0) < iota((LOW, LOW), 1)).astype(BF16)
    pltpu.matmul_push_rhs(upper, staging_register=0, mxu_index=0)
    pltpu.matmul_acc_lhs(acc, jnp.concatenate(hot, axis=0).astype(BF16), load_staged_rhs=0)
    inner = pltpu.matmul_pop(acc)
    rows, before = [], None
    for b in range(nblock):
        count = inner[b * nrows : (b + 1) * nrows]
        if before is not None:
            count = count + before
        row = jnp.sum(hot[b] * count, axis=0, keepdims=True)
        rows += [row[:, k : k + LANES] for k in range(0, LOW, LANES)]
        size = jnp.sum(hot[b], axis=1, keepdims=True)
        before = size if before is None else before + size
    return rows


def spill(out, values):
    for j in range(BLOCKS):
        start = j * LOW
        width = min(LOW, COLS - start)
        out[:, start : start + width] = values[j * ROWS_DEV : (j + 1) * ROWS_DEV, :width].astype(
            out.dtype
        )


def folded(row):
    lines = row.shape[1] // LANES
    return jnp.concatenate([row[:, k * LANES : (k + 1) * LANES] for k in range(lines)], axis=0)


def take(row, lane):
    return jnp.take_along_axis(
        jnp.broadcast_to(row, lane.shape), lane, axis=1, mode="promise_in_bounds"
    )


def packed(row):
    return jnp.broadcast_to(row, (PACK, row.shape[1])).astype(BF16)


def steps(first, period=PACK):
    return (iota((PACK, LANES), 0) % period + first).astype(F32).astype(BF16)


def low_hot(row, size):
    wide = packed(row)
    one, zero = jnp.ones((PACK, LANES), BF16), jnp.zeros((PACK, LANES), BF16)
    return jnp.concatenate(
        [jnp.where(steps(b) == wide, one, zero) for b in range(0, size, PACK)], axis=0
    )


def tiles_of(arrived, col_hot, slots):
    fields, lines = arrived.shape[1] - 1, arrived.shape[2]
    one, zero = jnp.ones((PACK, LANES), BF16), jnp.zeros((PACK, LANES), BF16)
    tiles = []
    for d in slots:
        cells = arrived[d, fields]
        high = jnp.floor(cells * (1.0 / LOW))
        low, high = cells - high * LOW, high - 1.0
        features = []
        for f in range(fields):
            x = arrived[d, f]
            features += [two(x), two(x * x)]
        for t in range(lines):
            hot = low_hot(low[t : t + 1], LOW)
            col_hot[d, :, t * LANES : (t + 1) * LANES] = hot
            quad = packed(high[t : t + 1])
            pairs = [
                jnp.concatenate(
                    [jnp.broadcast_to(x[t : t + 1], (8, LANES)) for x in feature], axis=0
                ).astype(BF16)
                for feature in features
            ]
            rows = []
            for j in range(0, QS, 8):
                here = steps(j, 8) == quad
                rows += [jnp.where(here, x, zero) for x in pairs]
            for j in range(0, QS, PACK):
                rows.append(jnp.where(steps(j) == quad, one, zero))
            tiles.append([jnp.concatenate(rows, axis=0), hot])
    return tiles


def grids_of(total, fields):
    out = []
    for p in range(2 * fields):
        rows = []
        for j in range(QS // 8):
            at = (j * 2 * fields + p) * 16
            rows.append(total[at : at + 8] + total[at + 8 : at + 16])
        out.append(jnp.concatenate(rows, axis=0))
    at = QS // 8 * 2 * fields * 16
    return total[at : at + QS], out[0::2], out[1::2]


def kernel(
    nrows,
    nchan,
    rad_in,
    band_in,
    rib_in,
    col_in,
    cnt_out,
    mean_out,
    var_out,
    spr_out,
    dep_out,
    rad_ref,
    band_ref,
    rib_ref,
    col_ref,
    staged,
    sent,
    arrived,
    col_hot,
    part_s,
    part_r,
    pairs,
    back_s,
    back_r,
    scale_r,
    turned,
    ready,
    ins,
    so,
    ro,
    sp,
    rp,
    sg,
    rg,
    sb,
    rb,
    ss,
    rs,
):
    me = lax.axis_index("rows")
    mc = lax.axis_index("chan")
    fields, obs = rad_ref.shape
    cap = 2 * obs // nrows
    lines = cap // LANES
    npair = nchan // 2
    far = list(range(nrows - 1, 0, -1))
    row_peer = [flip(me, d) for d in range(nrows)]
    chan_peer = [lax.rem(mc + 2 * j, nchan) for j in range(npair)]
    partner = flip(mc, 1)

    def remote(src, dst, send, recv, **to):
        return pltpu.make_async_remote_copy(
            src_ref=src,
            dst_ref=dst,
            send_sem=send,
            recv_sem=recv,
            device_id=to,
            device_id_type=MESH,
        )

    barrier = pltpu.get_barrier_semaphore()
    for d in far:
        pl.semaphore_signal(
            barrier, inc=1, device_id={"rows": row_peer[d]}, device_id_type=MESH
        )
    for e in range(1, nchan):
        pl.semaphore_signal(barrier, inc=1, device_id={"chan": flip(mc, e)}, device_id_type=MESH)
    fetches = [
        pltpu.make_async_copy(a, b, ins.at[i])
        for i, (a, b) in enumerate(
            ((band_in, band_ref), (rad_in, rad_ref), (rib_in, rib_ref), (col_in, col_ref))
        )
    ]
    for fetch in fetches:
        fetch.start()

    fetches[0].wait()
    dest = band_ref[...]

    def place_all(acc_rank, *accs):
        ranks = rank_of(dest, nrows, acc_rank)
        rank = folded(jnp.concatenate(ranks, axis=1)).astype(jnp.int32)
        wide = min(cap, LOW)
        parts = cap // wide
        hots, keys = [], []
        for k in range(obs // LANES):
            upper = jnp.floor(ranks[k] * (1.0 / wide))
            hots.append(low_hot(ranks[k] - upper * wide, LOW))
            names = jnp.bitwise_xor(dest[:, k * LANES : (k + 1) * LANES], me)
            keys.append(packed(names.astype(F32) * parts + upper))
        for fetch in fetches[1:]:
            fetch.wait()
        high, rest = two(rad_ref[...])
        middle, low = two(rest)
        col = col_ref[...]
        code = (col // LOW) * ROWS_DEV + rib_ref[...] + 1
        payload = jnp.concatenate(
            [high, middle, low]
            + [code.astype(F32), (col & (LOW - 1)).astype(F32)]
            + [jnp.zeros((PACK - 3 * fields - 2, obs), F32)],
            axis=0,
        ).astype(BF16)
        zero = jnp.zeros((PACK, LANES), BF16)
        left = []
        for k in range(obs // LANES):
            load = payload[:, k * LANES : (k + 1) * LANES]
            left.append(
                jnp.concatenate(
                    [
                        jnp.where(keys[k] == jnp.full((PACK, LANES), key, BF16), load, zero)
                        for key in range(nrows * parts)
                    ],
                    axis=0,
                )
            )
        product(accs, [list(x) for x in zip(left, hots)], True)
        placed = pltpu.matmul_pop(accs[0]) + pltpu.matmul_pop(accs[1])
        for d in far + [0]:
            target = sent if d > 0 else arrived
            for p in range(parts):
                part = placed[(d * parts + p) * PACK : (d * parts + p + 1) * PACK]
                values = (part[:fields] + part[fields : 2 * fields]) + part[2 * fields : 3 * fields]
                cells = part[3 * fields : 3 * fields + 1] * LOW + part[3 * fields + 1 : 3 * fields + 2]
                for i in range(wide // LANES):
                    t = p * (wide // LANES) + i
                    span = slice(i * LANES, (i + 1) * LANES)
                    at = (d * lines + t) * 8
                    staged[at : at + fields] = values[:, span]
                    staged[at + fields : at + fields + 1] = cells[:, span]
            for f in range(fields + 1):
                target[d, f] = staged[pl.ds(d * lines * 8 + f, lines, stride=8), :]
        return rank

    rows_placed = nrows * max(1, cap // LOW) * PACK
    rank = pl.run_scoped(
        place_all,
        pltpu.ACC(0)((nrows * obs // LOW, LOW), F32),
        pltpu.ACC(0)((rows_placed, LOW), F32),
        pltpu.ACC(1)((rows_placed, LOW), F32),
    )
    pl.semaphore_wait(barrier, nrows + nchan - 2)
    out_copies = {}
    for d in far:
        out_copies[d] = remote(
            sent.at[d], arrived.at[d], so.at[d], ro.at[d], rows=row_peer[d]
        )
        out_copies[d].start()
    for e in range(1, nchan):
        pl.semaphore_signal(ready, inc=1, device_id={"chan": flip(mc, e)}, device_id_type=MESH)

    half_rows = nrows // 2
    back_copies = {}

    def cells_all(acc_0, acc_1, *looks):
        accs = (acc_0, acc_1)
        groups = [[0], list(range(1, half_rows)), list(range(half_rows, nrows))]
        for slots in groups:
            for d in slots:
                if d > 0:
                    out_copies[d].wait_recv()
            product(accs, tiles_of(arrived, col_hot, slots), True)

        total = pltpu.matmul_pop(accs[0]) + pltpu.matmul_pop(accs[1])
        count, firsts, seconds = grids_of(total, fields)
        inverse = 1.0 / jnp.maximum(count, 1.0)
        partial = None
        means, variances = [], []
        for f in range(fields):
            mean = firsts[f] * inverse
            variance = jnp.maximum(seconds[f] * inverse - mean * mean, 0.0)
            means.append(mean)
            variances.append(variance)
            partial = variance if partial is None else partial + variance

        split = [two(x) for x in means + [partial]]
        pad = jnp.zeros((-(fields + 1) * QS % PACK, LOW), F32)
        table = [jnp.concatenate([x[k] for x in split] + [pad], axis=0).astype(BF16) for k in (0, 1)]
        places = [(d, t) for d in far + [0] for t in range(lines)]
        tiles = [places[i : i + 2] for i in range(0, len(places), 2)]

        def issue(i):
            register = i // 2 % 2
            hot = jnp.concatenate(
                [col_hot[d, :, t * LANES : (t + 1) * LANES] for d, t in tiles[i]], axis=1
            )
            acc = looks[i % len(looks)]
            pltpu.matmul_push_rhs(hot, staging_register=register, mxu_index=i % 2)
            pltpu.matmul_acc_lhs(acc, table[0], load_staged_rhs=register)
            pltpu.matmul_acc_lhs(acc, table[1])

        pl.semaphore_wait(ready, nchan - 1)
        scale_copies = []
        for i in range(min(len(looks), len(tiles))):
            issue(i)
        for i, tile in enumerate(tiles):
            picked = pltpu.matmul_pop(looks[i % len(looks)])
            if i + len(looks) < len(tiles):
                issue(i + len(looks))
            for k, (d, t) in enumerate(tile):
                span = slice(k * LANES, (k + 1) * LANES)
                target = back_s if d > 0 else back_r
                high = arrived[d, fields, t : t + 1].astype(jnp.int32) // LOW - 1
                here = iota((QS, LANES), 0) == high
                for f in range(fields + 1):
                    both = picked[f * QS : (f + 1) * QS, span]
                    found = jnp.sum(jnp.where(here, both, 0.0), axis=0, keepdims=True)
                    if f < fields:
                        target[d, f, t : t + 1] = arrived[d, f, t : t + 1] - found
                    else:
                        target[d, f, t : t + 1] = found
                if t < lines - 1:
                    continue
                for e in range(nchan - 1, 0, -1):
                    slot = e * nrows + d
                    copy = remote(
                        target.at[d, fields],
                        scale_r.at[slot],
                        ss.at[slot],
                        rs.at[slot],
                        rows=row_peer[d],
                        chan=flip(mc, e),
                    )
                    copy.start()
                    scale_copies.append((d, copy))
                if d > 0:
                    back_copies[d] = remote(
                        back_s.at[d], back_r.at[d], sb.at[d], rb.at[d], rows=row_peer[d]
                    )
                    back_copies[d].start()
        part_s[...] = partial
        part_copy = remote(part_s, part_r, sp.at[0], rp.at[0], chan=partner)
        part_copy.start()

        spill(cnt_out, count)
        for f in range(fields):
            spill(mean_out.at[f], means[f])
            spill(var_out.at[f], variances[f])
        part_copy.wait_recv()
        mine = mc // 2
        pairs[mine] = part_s[...] + part_r[...]
        pair_copies = []
        for j in range(1, npair):
            copy = remote(pairs.at[mine], pairs.at[mine], sg.at[j], rg.at[j], chan=chan_peer[j])
            copy.start()
            pair_copies.append(copy)

        place = jnp.bitwise_xor(folded(dest), me) * lines + rank // LANES
        lane = rank & (LANES - 1)
        found = [jnp.zeros(rank.shape, F32) for _ in range(fields + 1)]
        far_half = list(range(nrows - 1, half_rows - 1, -1))
        returns = [list(range(half_rows)), far_half]
        for slots in returns:
            for d in slots:
                if d > 0:
                    back_copies[d].wait_recv()
            for d in slots:
                for t in range(lines):
                    here = place == d * lines + t
                    for f in range(fields):
                        found[f] = jnp.where(here, take(back_r[d, f, t : t + 1], lane), found[f])
        for slots in returns:
            for d, copy in scale_copies:
                if d in slots:
                    copy.wait_recv()
            for d in slots:
                for t in range(lines):
                    here = place == d * lines + t
                    row = back_r[d, fields, t : t + 1]
                    for e in range(1, nchan):
                        row = row + scale_r[e * nrows + d, t : t + 1]
                    found[fields] = jnp.where(here, take(row, lane), found[fields])
        scale = lax.rsqrt(1.0 + found[fields] / CHAN)
        many = obs // LANES
        for f in range(fields):
            turned[f * many : (f + 1) * many] = found[f] * scale
        for k in range(many):
            dep_out[:, k * LANES : (k + 1) * LANES] = turned[pl.ds(k, fields, stride=many), :]
        for copy in pair_copies:
            copy.wait_recv()
        spread = pairs[0]
        for p in range(1, npair):
            spread = spread + pairs[p]
        spill(spr_out, spread)

        for copies in (out_copies, back_copies):
            for copy in copies.values():
                copy.wait_send()
        for copy in [part_copy] + pair_copies + [copy for _, copy in scale_copies]:
            copy.wait_send()

    rows_summed = QS * 4 * fields + -(-QS // PACK) * PACK
    rows_looked = -(-(fields + 1) * QS // PACK) * PACK
    pl.run_scoped(
        cells_all,
        *(pltpu.ACC(unit)((rows_summed, LOW), F32) for unit in (0, 1)),
        *(pltpu.ACC(unit)((rows_looked, LOW), F32) for unit in (0, 1) * 4),
    )


def finish(*refs):
    half = (len(refs) - 1) // 2
    sems = refs[-1]
    copies = [
        pltpu.make_async_copy(a, b, sems.at[i])
        for i, (a, b) in enumerate(zip(refs[:half], refs[half : 2 * half]))
    ]
    for copy in copies:
        copy.start()
    for copy in copies:
        copy.wait()


def body(radiances, band, row_in_band, column):
    nrows = lax.axis_size("rows")
    nchan = lax.axis_size("chan")
    fields, obs = radiances.shape
    cap = 2 * obs // nrows
    lines = cap // LANES
    npair = nchan // 2
    vmem = pl.BlockSpec(memory_space=pltpu.VMEM)
    anywhere = pl.BlockSpec(memory_space=pl.ANY)
    dma = pltpu.SemaphoreType.DMA
    shapes = (
        ((ROWS_DEV, COLS), jnp.int32),
        ((fields, ROWS_DEV, COLS), F32),
        ((fields, ROWS_DEV, COLS), F32),
        ((ROWS_DEV, COLS), F32),
        ((fields, obs), F32),
    )
    held = pl.pallas_call(
        functools.partial(kernel, nrows, nchan),
        out_shape=tuple(pltpu.VMEM(s, t) for s, t in shapes),
        in_specs=[pl.BlockSpec(memory_space=pltpu.HBM)] * 4,
        out_specs=(vmem,) * len(shapes),
        scratch_shapes=[
            pltpu.VMEM((fields, obs), F32),
            pltpu.VMEM((1, obs), jnp.int32),
            pltpu.VMEM((1, obs), jnp.int32),
            pltpu.VMEM((1, obs), jnp.int32),
            pltpu.VMEM((nrows * lines * 8, LANES), F32),
            pltpu.VMEM((nrows, fields + 1, lines, LANES), F32),
            pltpu.VMEM((nrows, fields + 1, lines, LANES), F32),
            pltpu.VMEM((nrows, LOW, cap), BF16),
            pltpu.VMEM((QS, LOW), F32),
            pltpu.VMEM((QS, LOW), F32),
            pltpu.VMEM((npair, QS, LOW), F32),
            pltpu.VMEM((nrows, fields + 1, lines, LANES), F32),
            pltpu.VMEM((nrows, fields + 1, lines, LANES), F32),
            pltpu.VMEM((nchan * nrows, lines, LANES), F32),
            pltpu.VMEM((fields * obs // LANES, LANES), F32),
            pltpu.SemaphoreType.REGULAR,
            dma((4,)),
            dma((nrows,)),
            dma((nrows,)),
            dma((1,)),
            dma((1,)),
            dma((npair,)),
            dma((npair,)),
            dma((nrows,)),
            dma((nrows,)),
            dma((nchan * nrows,)),
            dma((nchan * nrows,)),
        ],
        compiler_params=pltpu.CompilerParams(
            collective_id=0, has_side_effects=True, vmem_limit_bytes=32 * 1024 * 1024
        ),
    )(
        *(
            pltpu.with_memory_space_constraint(x, pltpu.HBM)
            for x in (
                radiances,
                band.reshape(1, obs),
                row_in_band.reshape(1, obs),
                column.reshape(1, obs),
            )
        )
    )
    return pl.pallas_call(
        finish,
        out_shape=tuple(jax.ShapeDtypeStruct(s, t) for s, t in shapes),
        in_specs=[vmem] * len(shapes),
        out_specs=(anywhere,) * len(shapes),
        scratch_shapes=[dma((len(shapes),))],
        compiler_params=pltpu.CompilerParams(vmem_limit_bytes=32 * 1024 * 1024),
    )(*held)


def solution(mesh):
    in_specs = (P("chan", "rows"), P("rows", None), P("rows"), P("rows"))
    out_specs = (
        P("rows", None),
        P("chan", "rows", None),
        P("chan", "rows", None),
        P("rows", None),
        P("chan", "rows"),
    )
    return jax.shard_map(body, mesh=mesh, in_specs=in_specs, out_specs=out_specs, check_vma=False)
```

```python
import functools

import jax
import jax.numpy as jnp
from jax import lax
from jax.experimental import pallas as pl
from jax.experimental.pallas import tpu as pltpu
from jax.sharding import PartitionSpec as P

CHAN = 16
PACK = 16
COLS = 1440
ROWS_DEV = 4
LOW = 256
LANES = 128
BLOCKS = -(-COLS // LOW)
QS = BLOCKS * ROWS_DEV
F32 = jnp.float32
BF16 = jnp.bfloat16
MESH = pl.DeviceIdType.MESH
NT = (((1,), (1,)), ((), ()))
NN = (((1,), (0,)), ((), ()))


def iota(shape, axis):
    return lax.broadcasted_iota(jnp.int32, shape, axis)


def onehot(mask):
    return jnp.where(mask, 1.0, 0.0)


def two(values):
    high = values.astype(BF16).astype(F32)
    return high, values - high


def product(accs, tiles, transpose):
    for i in range(0, len(tiles), 2):
        pair = tiles[i : i + 2]
        if len(pair) < 2:
            pair.append([jnp.zeros_like(x) for x in pair[0]])
        left, right = (jnp.concatenate(x, axis=1) for x in zip(*pair))
        unit, register = i // 2 % 2, i // 4 % 2
        pltpu.matmul_push_rhs(
            right, staging_register=register, mxu_index=unit, transpose=transpose
        )
        pltpu.matmul_acc_lhs(accs[unit], left, load_staged_rhs=register)


def flip(index, bits):
    out, bit = index, 1
    while bit <= bits:
        if bits & bit:
            out = out + bit - 2 * bit * ((index // bit) % 2)
        bit *= 2
    return out


def rank_of(dest, nrows, acc):
    obs = dest.shape[1]
    nblock = obs // LOW
    hot = [
        onehot(iota((nrows, LOW), 0) == dest[:, b * LOW : (b + 1) * LOW]) for b in range(nblock)
    ]
    upper = onehot(iota((LOW, LOW), 0) < iota((LOW, LOW), 1)).astype(BF16)
    pltpu.matmul_push_rhs(upper, staging_register=0, mxu_index=0)
    pltpu.matmul_acc_lhs(acc, jnp.concatenate(hot, axis=0).astype(BF16), load_staged_rhs=0)
    inner = pltpu.matmul_pop(acc)
    rows, before = [], None
    for b in range(nblock):
        count = inner[b * nrows : (b + 1) * nrows]
        if before is not None:
            count = count + before
        row = jnp.sum(hot[b] * count, axis=0, keepdims=True)
        rows += [row[:, k : k + LANES] for k in range(0, LOW, LANES)]
        size = jnp.sum(hot[b], axis=1, keepdims=True)
        before = size if before is None else before + size
    return rows


def spill(out, values):
    for j in range(BLOCKS):
        start = j * LOW
        width = min(LOW, COLS - start)
        out[:, start : start + width] = values[j * ROWS_DEV : (j + 1) * ROWS_DEV, :width].astype(
            out.dtype
        )


def folded(row):
    lines = row.shape[1] // LANES
    return jnp.concatenate([row[:, k * LANES : (k + 1) * LANES] for k in range(lines)], axis=0)


def take(row, lane):
    return jnp.take_along_axis(
        jnp.broadcast_to(row, lane.shape), lane, axis=1, mode="promise_in_bounds"
    )


def packed(row):
    return jnp.broadcast_to(row, (PACK, row.shape[1])).astype(BF16)


def steps(first, period=PACK):
    return (iota((PACK, LANES), 0) % period + first).astype(F32).astype(BF16)


def low_hot(row, size):
    wide = packed(row)
    one, zero = jnp.ones((PACK, LANES), BF16), jnp.zeros((PACK, LANES), BF16)
    return jnp.concatenate(
        [jnp.where(steps(b) == wide, one, zero) for b in range(0, size, PACK)], axis=0
    )


def tiles_of(arrived, col_hot, slots):
    fields, lines = arrived.shape[1] - 1, arrived.shape[2]
    one, zero = jnp.ones((PACK, LANES), BF16), jnp.zeros((PACK, LANES), BF16)
    tiles = []
    for d in slots:
        cells = arrived[d, fields]
        high = jnp.floor(cells * (1.0 / LOW))
        low, high = cells - high * LOW, high - 1.0
        features = []
        for f in range(fields):
            x = arrived[d, f]
            features += [two(x), two(x * x)]
        for t in range(lines):
            hot = low_hot(low[t : t + 1], LOW)
            col_hot[d, :, t * LANES : (t + 1) * LANES] = hot
            quad = packed(high[t : t + 1])
            pairs = [
                jnp.concatenate(
                    [jnp.broadcast_to(x[t : t + 1], (8, LANES)) for x in feature], axis=0
                ).astype(BF16)
                for feature in features
            ]
            rows = []
            for j in range(0, QS, 8):
                here = steps(j, 8) == quad
                rows += [jnp.where(here, x, zero) for x in pairs]
            for j in range(0, QS, PACK):
                rows.append(jnp.where(steps(j) == quad, one, zero))
            tiles.append([jnp.concatenate(rows, axis=0), hot])
    return tiles


def grids_of(total, fields):
    out = []
    for p in range(2 * fields):
        rows = []
        for j in range(QS // 8):
            at = (j * 2 * fields + p) * 16
            rows.append(total[at : at + 8] + total[at + 8 : at + 16])
        out.append(jnp.concatenate(rows, axis=0))
    at = QS // 8 * 2 * fields * 16
    return total[at : at + QS], out[0::2], out[1::2]


def kernel(
    nrows,
    nchan,
    rad_in,
    band_in,
    rib_in,
    col_in,
    cnt_out,
    mean_out,
    var_out,
    spr_out,
    dep_out,
    rad_ref,
    band_ref,
    rib_ref,
    col_ref,
    staged,
    sent,
    arrived,
    col_hot,
    part_s,
    part_r,
    pairs,
    back_s,
    back_r,
    scale_r,
    turned,
    ready,
    ins,
    send,
    came,
    back,
    scales,
    shares,
):
    me = lax.axis_index("rows")
    mc = lax.axis_index("chan")
    fields, obs = rad_ref.shape
    cap = 2 * obs // nrows
    lines = cap // LANES
    npair = nchan // 2
    half_rows = nrows // 2
    far = list(range(nrows - 1, 0, -1))
    row_peer = [flip(me, d) for d in range(nrows)]
    chan_peer = [lax.rem(mc + 2 * j, nchan) for j in range(npair)]
    partner = flip(mc, 1)

    def wait_all(ref, semaphore):
        pltpu.make_async_copy(ref, ref, semaphore).wait()

    def remote(src, dst, kind, recv, **to):
        return pltpu.make_async_remote_copy(
            src_ref=src,
            dst_ref=dst,
            send_sem=send.at[kind],
            recv_sem=recv,
            device_id=to,
            device_id_type=MESH,
        )

    barrier = pltpu.get_barrier_semaphore()
    for d in far:
        pl.semaphore_signal(
            barrier, inc=1, device_id={"rows": row_peer[d]}, device_id_type=MESH
        )
    for e in range(1, nchan):
        pl.semaphore_signal(barrier, inc=1, device_id={"chan": flip(mc, e)}, device_id_type=MESH)
    fetches = [
        pltpu.make_async_copy(a, b, ins.at[i])
        for i, (a, b) in enumerate(
            ((band_in, band_ref), (rad_in, rad_ref), (rib_in, rib_ref), (col_in, col_ref))
        )
    ]
    for fetch in fetches:
        fetch.start()

    fetches[0].wait()
    dest = band_ref[...]

    def place_all(acc_rank, *accs):
        ranks = rank_of(dest, nrows, acc_rank)
        rank = folded(jnp.concatenate(ranks, axis=1)).astype(jnp.int32)
        wide = min(cap, LOW)
        parts = cap // wide
        hots, keys = [], []
        for k in range(obs // LANES):
            upper = jnp.floor(ranks[k] * (1.0 / wide))
            hots.append(low_hot(ranks[k] - upper * wide, LOW))
            names = jnp.bitwise_xor(dest[:, k * LANES : (k + 1) * LANES], me)
            keys.append(packed(names.astype(F32) * parts + upper))
        for fetch in fetches[1:]:
            fetch.wait()
        high, rest = two(rad_ref[...])
        middle, low = two(rest)
        col = col_ref[...]
        code = (col // LOW) * ROWS_DEV + rib_ref[...] + 1
        payload = jnp.concatenate(
            [high, middle, low]
            + [code.astype(F32), (col & (LOW - 1)).astype(F32)]
            + [jnp.zeros((PACK - 3 * fields - 2, obs), F32)],
            axis=0,
        ).astype(BF16)
        zero = jnp.zeros((PACK, LANES), BF16)
        left = []
        for k in range(obs // LANES):
            load = payload[:, k * LANES : (k + 1) * LANES]
            left.append(
                jnp.concatenate(
                    [
                        jnp.where(keys[k] == jnp.full((PACK, LANES), key, BF16), load, zero)
                        for key in range(nrows * parts)
                    ],
                    axis=0,
                )
            )
        product(accs, [list(x) for x in zip(left, hots)], True)
        placed = pltpu.matmul_pop(accs[0]) + pltpu.matmul_pop(accs[1])
        for d in far + [0]:
            target = sent if d > 0 else arrived
            for p in range(parts):
                part = placed[(d * parts + p) * PACK : (d * parts + p + 1) * PACK]
                values = (part[:fields] + part[fields : 2 * fields]) + part[2 * fields : 3 * fields]
                cells = part[3 * fields : 3 * fields + 1] * LOW + part[3 * fields + 1 : 3 * fields + 2]
                for i in range(wide // LANES):
                    t = p * (wide // LANES) + i
                    span = slice(i * LANES, (i + 1) * LANES)
                    at = (d * lines + t) * 8
                    staged[at : at + fields] = values[:, span]
                    staged[at + fields : at + fields + 1] = cells[:, span]
            for f in range(fields + 1):
                target[d, f] = staged[pl.ds(d * lines * 8 + f, lines, stride=8), :]
        return rank

    rows_placed = nrows * max(1, cap // LOW) * PACK
    rank = pl.run_scoped(
        place_all,
        pltpu.ACC(0)((nrows * obs // LOW, LOW), F32),
        pltpu.ACC(0)((rows_placed, LOW), F32),
        pltpu.ACC(1)((rows_placed, LOW), F32),
    )
    pl.semaphore_wait(barrier, nrows + nchan - 2)
    for d in far:
        remote(
            sent.at[d], arrived.at[d], 0, came.at[d // half_rows], rows=row_peer[d]
        ).start()
    for e in range(1, nchan):
        pl.semaphore_signal(ready, inc=1, device_id={"chan": flip(mc, e)}, device_id_type=MESH)


    def cells_all(acc_0, acc_1, *looks):
        accs = (acc_0, acc_1)
        groups = [[0], list(range(1, half_rows)), list(range(half_rows, nrows))]
        for slots in groups:
            if slots[0] > 0:
                wait_all(arrived.at[slots[0] : slots[-1] + 1], came.at[slots[0] // half_rows])
            product(accs, tiles_of(arrived, col_hot, slots), True)

        total = pltpu.matmul_pop(accs[0]) + pltpu.matmul_pop(accs[1])
        count, firsts, seconds = grids_of(total, fields)
        inverse = 1.0 / jnp.maximum(count, 1.0)
        partial = None
        means, variances = [], []
        for f in range(fields):
            mean = firsts[f] * inverse
            variance = jnp.maximum(seconds[f] * inverse - mean * mean, 0.0)
            means.append(mean)
            variances.append(variance)
            partial = variance if partial is None else partial + variance

        split = [two(x) for x in means + [partial]]
        pad = jnp.zeros((-(fields + 1) * QS % PACK, LOW), F32)
        table = [jnp.concatenate([x[k] for x in split] + [pad], axis=0).astype(BF16) for k in (0, 1)]
        places = [(d, t) for d in far + [0] for t in range(lines)]
        tiles = [places[i : i + 2] for i in range(0, len(places), 2)]

        def issue(i):
            register = i // 2 % 2
            hot = jnp.concatenate(
                [col_hot[d, :, t * LANES : (t + 1) * LANES] for d, t in tiles[i]], axis=1
            )
            acc = looks[i % len(looks)]
            pltpu.matmul_push_rhs(hot, staging_register=register, mxu_index=i % 2)
            pltpu.matmul_acc_lhs(acc, table[0], load_staged_rhs=register)
            pltpu.matmul_acc_lhs(acc, table[1])

        pl.semaphore_wait(ready, nchan - 1)
        for i in range(min(len(looks), len(tiles))):
            issue(i)
        for i, tile in enumerate(tiles):
            picked = pltpu.matmul_pop(looks[i % len(looks)])
            if i + len(looks) < len(tiles):
                issue(i + len(looks))
            for k, (d, t) in enumerate(tile):
                span = slice(k * LANES, (k + 1) * LANES)
                target = back_s if d > 0 else back_r
                high = arrived[d, fields, t : t + 1].astype(jnp.int32) // LOW - 1
                here = iota((QS, LANES), 0) == high
                for f in range(fields + 1):
                    both = picked[f * QS : (f + 1) * QS, span]
                    found = jnp.sum(jnp.where(here, both, 0.0), axis=0, keepdims=True)
                    if f < fields:
                        target[d, f, t : t + 1] = arrived[d, f, t : t + 1] - found
                    else:
                        target[d, f, t : t + 1] = found
                if t < lines - 1:
                    continue
                for e in range(nchan - 1, 0, -1):
                    slot = e * nrows + d
                    remote(
                        target.at[d, fields],
                        scale_r.at[slot],
                        2,
                        scales.at[d // half_rows],
                        rows=row_peer[d],
                        chan=flip(mc, e),
                    ).start()
                if d > 0:
                    remote(
                        back_s.at[d], back_r.at[d], 1, back.at[d // half_rows], rows=row_peer[d]
                    ).start()
        part_s[...] = partial
        part_copy = remote(part_s, part_r, 3, shares.at[0], chan=partner)
        part_copy.start()

        spill(cnt_out, count)
        for f in range(fields):
            spill(mean_out.at[f], means[f])
            spill(var_out.at[f], variances[f])
        part_copy.wait_recv()
        mine = mc // 2
        pairs[mine] = part_s[...] + part_r[...]
        for j in range(1, npair):
            remote(pairs.at[mine], pairs.at[mine], 4, shares.at[1], chan=chan_peer[j]).start()

        place = jnp.bitwise_xor(folded(dest), me) * lines + rank // LANES
        lane = rank & (LANES - 1)
        found = [jnp.zeros(rank.shape, F32) for _ in range(fields + 1)]
        far_half = list(range(nrows - 1, half_rows - 1, -1))
        returns = [list(range(half_rows)), far_half]
        for slots in returns:
            first = max(1, min(slots))
            wait_all(back_r.at[first : max(slots) + 1], back.at[first // half_rows])
            for d in slots:
                for t in range(lines):
                    here = place == d * lines + t
                    for f in range(fields):
                        found[f] = jnp.where(here, take(back_r[d, f, t : t + 1], lane), found[f])
        for slots in returns:
            wait_all(
                scale_r.at[nrows : nrows + (nchan - 1) * len(slots)],
                scales.at[slots[0] // half_rows],
            )
            for d in slots:
                for t in range(lines):
                    here = place == d * lines + t
                    row = back_r[d, fields, t : t + 1]
                    for e in range(1, nchan):
                        row = row + scale_r[e * nrows + d, t : t + 1]
                    found[fields] = jnp.where(here, take(row, lane), found[fields])
        scale = lax.rsqrt(1.0 + found[fields] / CHAN)
        many = obs // LANES
        for f in range(fields):
            turned[f * many : (f + 1) * many] = found[f] * scale
        for k in range(many):
            dep_out[:, k * LANES : (k + 1) * LANES] = turned[pl.ds(k, fields, stride=many), :]
        wait_all(pairs.at[1:], shares.at[1])
        spread = pairs[0]
        for p in range(1, npair):
            spread = spread + pairs[p]
        spill(spr_out, spread)

        wait_all(sent.at[1:], send.at[0])
        wait_all(back_s.at[1:], send.at[1])
        wait_all(scale_r.at[nrows:], send.at[2])
        part_copy.wait_send()
        wait_all(pairs.at[1:], send.at[4])

    rows_summed = QS * 4 * fields + -(-QS // PACK) * PACK
    rows_looked = -(-(fields + 1) * QS // PACK) * PACK
    pl.run_scoped(
        cells_all,
        *(pltpu.ACC(unit)((rows_summed, LOW), F32) for unit in (0, 1)),
        *(pltpu.ACC(unit)((rows_looked, LOW), F32) for unit in (0, 1) * 4),
    )


def finish(*refs):
    half = (len(refs) - 1) // 2
    sems = refs[-1]
    copies = [
        pltpu.make_async_copy(a, b, sems.at[i])
        for i, (a, b) in enumerate(zip(refs[:half], refs[half : 2 * half]))
    ]
    for copy in copies:
        copy.start()
    for copy in copies:
        copy.wait()


def body(radiances, band, row_in_band, column):
    nrows = lax.axis_size("rows")
    nchan = lax.axis_size("chan")
    fields, obs = radiances.shape
    cap = 2 * obs // nrows
    lines = cap // LANES
    npair = nchan // 2
    vmem = pl.BlockSpec(memory_space=pltpu.VMEM)
    anywhere = pl.BlockSpec(memory_space=pl.ANY)
    dma = pltpu.SemaphoreType.DMA
    shapes = (
        ((ROWS_DEV, COLS), jnp.int32),
        ((fields, ROWS_DEV, COLS), F32),
        ((fields, ROWS_DEV, COLS), F32),
        ((ROWS_DEV, COLS), F32),
        ((fields, obs), F32),
    )
    held = pl.pallas_call(
        functools.partial(kernel, nrows, nchan),
        out_shape=tuple(pltpu.VMEM(s, t) for s, t in shapes),
        in_specs=[pl.BlockSpec(memory_space=pltpu.HBM)] * 4,
        out_specs=(vmem,) * len(shapes),
        scratch_shapes=[
            pltpu.VMEM((fields, obs), F32),
            pltpu.VMEM((1, obs), jnp.int32),
            pltpu.VMEM((1, obs), jnp.int32),
            pltpu.VMEM((1, obs), jnp.int32),
            pltpu.VMEM((nrows * lines * 8, LANES), F32),
            pltpu.VMEM((nrows, fields + 1, lines, LANES), F32),
            pltpu.VMEM((nrows, fields + 1, lines, LANES), F32),
            pltpu.VMEM((nrows, LOW, cap), BF16),
            pltpu.VMEM((QS, LOW), F32),
            pltpu.VMEM((QS, LOW), F32),
            pltpu.VMEM((npair, QS, LOW), F32),
            pltpu.VMEM((nrows, fields + 1, lines, LANES), F32),
            pltpu.VMEM((nrows, fields + 1, lines, LANES), F32),
            pltpu.VMEM((nchan * nrows, lines, LANES), F32),
            pltpu.VMEM((fields * obs // LANES, LANES), F32),
            pltpu.SemaphoreType.REGULAR,
            dma((4,)),
            dma((5,)),
            dma((2,)),
            dma((2,)),
            dma((2,)),
            dma((2,)),
        ],
        compiler_params=pltpu.CompilerParams(
            collective_id=0, has_side_effects=True, vmem_limit_bytes=32 * 1024 * 1024
        ),
    )(
        *(
            pltpu.with_memory_space_constraint(x, pltpu.HBM)
            for x in (
                radiances,
                band.reshape(1, obs),
                row_in_band.reshape(1, obs),
                column.reshape(1, obs),
            )
        )
    )
    return pl.pallas_call(
        finish,
        out_shape=tuple(jax.ShapeDtypeStruct(s, t) for s, t in shapes),
        in_specs=[vmem] * len(shapes),
        out_specs=(anywhere,) * len(shapes),
        scratch_shapes=[dma((len(shapes),))],
        compiler_params=pltpu.CompilerParams(vmem_limit_bytes=32 * 1024 * 1024),
    )(*held)


def solution(mesh):
    in_specs = (P("chan", "rows"), P("rows", None), P("rows"), P("rows"))
    out_specs = (
        P("rows", None),
        P("chan", "rows", None),
        P("chan", "rows", None),
        P("rows", None),
        P("chan", "rows"),
    )
    return jax.shard_map(body, mesh=mesh, in_specs=in_specs, out_specs=out_specs, check_vma=False)
```

```python
import functools

import jax
import jax.numpy as jnp
from jax import lax
from jax.experimental import pallas as pl
from jax.experimental.pallas import tpu as pltpu
from jax.sharding import PartitionSpec as P

CHAN = 16
PACK = 16
COLS = 1440
ROWS_DEV = 4
LOW = 256
LANES = 128
BLOCKS = -(-COLS // LOW)
QS = BLOCKS * ROWS_DEV
F32 = jnp.float32
BF16 = jnp.bfloat16
MESH = pl.DeviceIdType.MESH
NT = (((1,), (1,)), ((), ()))
NN = (((1,), (0,)), ((), ()))


def iota(shape, axis):
    return lax.broadcasted_iota(jnp.int32, shape, axis)


def onehot(mask):
    return jnp.where(mask, 1.0, 0.0)


def two(values):
    high = values.astype(BF16).astype(F32)
    return high, values - high


def product(accs, tiles, transpose):
    for i in range(0, len(tiles), 2):
        pair = tiles[i : i + 2]
        if len(pair) < 2:
            pair.append([jnp.zeros_like(x) for x in pair[0]])
        left, right = (jnp.concatenate(x, axis=1) for x in zip(*pair))
        unit, register = i // 2 % 2, i // 4 % 2
        pltpu.matmul_push_rhs(
            right, staging_register=register, mxu_index=unit, transpose=transpose
        )
        pltpu.matmul_acc_lhs(accs[unit], left, load_staged_rhs=register)


def flip(index, bits):
    out, bit = index, 1
    while bit <= bits:
        if bits & bit:
            out = out + bit - 2 * bit * ((index // bit) % 2)
        bit *= 2
    return out


def rank_of(dest, nrows, acc):
    obs = dest.shape[1]
    nblock = obs // LOW
    hot = [
        onehot(iota((nrows, LOW), 0) == dest[:, b * LOW : (b + 1) * LOW]) for b in range(nblock)
    ]
    upper = onehot(iota((LOW, LOW), 0) < iota((LOW, LOW), 1)).astype(BF16)
    pltpu.matmul_push_rhs(upper, staging_register=0, mxu_index=0)
    pltpu.matmul_acc_lhs(acc, jnp.concatenate(hot, axis=0).astype(BF16), load_staged_rhs=0)
    inner = pltpu.matmul_pop(acc)
    rows, before = [], None
    for b in range(nblock):
        count = inner[b * nrows : (b + 1) * nrows]
        if before is not None:
            count = count + before
        row = jnp.sum(hot[b] * count, axis=0, keepdims=True)
        rows += [row[:, k : k + LANES] for k in range(0, LOW, LANES)]
        size = jnp.sum(hot[b], axis=1, keepdims=True)
        before = size if before is None else before + size
    return rows


def spill(out, values):
    for j in range(BLOCKS):
        start = j * LOW
        width = min(LOW, COLS - start)
        out[:, start : start + width] = values[j * ROWS_DEV : (j + 1) * ROWS_DEV, :width].astype(
            out.dtype
        )


def folded(row):
    lines = row.shape[1] // LANES
    return jnp.concatenate([row[:, k * LANES : (k + 1) * LANES] for k in range(lines)], axis=0)


def take(row, lane):
    return jnp.take_along_axis(
        jnp.broadcast_to(row, lane.shape), lane, axis=1, mode="promise_in_bounds"
    )


def packed(row):
    return jnp.broadcast_to(row, (PACK, row.shape[1])).astype(BF16)


def steps(first, period=PACK):
    return (iota((PACK, LANES), 0) % period + first).astype(F32).astype(BF16)


def low_hot(row, size):
    wide = packed(row)
    one, zero = jnp.ones((PACK, LANES), BF16), jnp.zeros((PACK, LANES), BF16)
    return jnp.concatenate(
        [jnp.where(steps(b) == wide, one, zero) for b in range(0, size, PACK)], axis=0
    )


def tiles_of(arrived, col_hot, slots):
    fields, lines = arrived.shape[1] - 1, arrived.shape[2]
    one, zero = jnp.ones((PACK, LANES), BF16), jnp.zeros((PACK, LANES), BF16)
    tiles = []
    for d in slots:
        cells = arrived[d, fields]
        high = jnp.floor(cells * (1.0 / LOW))
        low, high = cells - high * LOW, high - 1.0
        features = []
        for f in range(fields):
            x = arrived[d, f]
            features += [two(x), two(x * x)]
        for t in range(lines):
            hot = low_hot(low[t : t + 1], LOW)
            col_hot[d, :, t * LANES : (t + 1) * LANES] = hot
            quad = packed(high[t : t + 1])
            pairs = [
                jnp.concatenate(
                    [jnp.broadcast_to(x[t : t + 1], (8, LANES)) for x in feature], axis=0
                ).astype(BF16)
                for feature in features
            ]
            rows = []
            for j in range(0, QS, 8):
                here = steps(j, 8) == quad
                rows += [jnp.where(here, x, zero) for x in pairs]
            for j in range(0, QS, PACK):
                rows.append(jnp.where(steps(j) == quad, one, zero))
            tiles.append([jnp.concatenate(rows, axis=0), hot])
    return tiles


def grids_of(total, fields):
    out = []
    for p in range(2 * fields):
        rows = []
        for j in range(QS // 8):
            at = (j * 2 * fields + p) * 16
            rows.append(total[at : at + 8] + total[at + 8 : at + 16])
        out.append(jnp.concatenate(rows, axis=0))
    at = QS // 8 * 2 * fields * 16
    return total[at : at + QS], out[0::2], out[1::2]


def kernel(
    nrows,
    nchan,
    rad_in,
    band_in,
    rib_in,
    col_in,
    cnt_out,
    mean_out,
    var_out,
    spr_out,
    dep_out,
    rad_ref,
    band_ref,
    rib_ref,
    col_ref,
    staged,
    sent,
    arrived,
    col_hot,
    part_s,
    part_r,
    pairs,
    back_s,
    back_r,
    scale_r,
    turned,
    ready,
    ins,
    send,
    came,
    back,
    scales,
    shares,
):
    me = lax.axis_index("rows")
    mc = lax.axis_index("chan")
    fields, obs = rad_ref.shape
    cap = 2 * obs // nrows
    lines = cap // LANES
    npair = nchan // 2
    half_rows = nrows // 2
    far = sorted(range(1, nrows), key=lambda d: (d // half_rows, d % 2, d), reverse=True)
    row_peer = [flip(me, d) for d in range(nrows)]
    chan_peer = [lax.rem(mc + 2 * j, nchan) for j in range(npair)]
    partner = flip(mc, 1)

    def wait_all(ref, semaphore):
        pltpu.make_async_copy(ref, ref, semaphore).wait()

    def remote(src, dst, kind, recv, **to):
        return pltpu.make_async_remote_copy(
            src_ref=src,
            dst_ref=dst,
            send_sem=send.at[kind],
            recv_sem=recv,
            device_id=to,
            device_id_type=MESH,
        )

    barrier = pltpu.get_barrier_semaphore()
    for d in far:
        pl.semaphore_signal(
            barrier, inc=1, device_id={"rows": row_peer[d]}, device_id_type=MESH
        )
    for e in range(1, nchan):
        pl.semaphore_signal(barrier, inc=1, device_id={"chan": flip(mc, e)}, device_id_type=MESH)
    fetches = [
        pltpu.make_async_copy(a, b, ins.at[i])
        for i, (a, b) in enumerate(
            ((band_in, band_ref), (rad_in, rad_ref), (rib_in, rib_ref), (col_in, col_ref))
        )
    ]
    for fetch in fetches:
        fetch.start()

    fetches[0].wait()
    dest = band_ref[...]

    def place_all(acc_rank, *accs):
        ranks = rank_of(dest, nrows, acc_rank)
        rank = folded(jnp.concatenate(ranks, axis=1)).astype(jnp.int32)
        wide = min(cap, LOW)
        parts = cap // wide
        hots, keys = [], []
        for k in range(obs // LANES):
            upper = jnp.floor(ranks[k] * (1.0 / wide))
            hots.append(low_hot(ranks[k] - upper * wide, LOW))
            names = jnp.bitwise_xor(dest[:, k * LANES : (k + 1) * LANES], me)
            keys.append(packed(names.astype(F32) * parts + upper))
        for fetch in fetches[1:]:
            fetch.wait()
        high, rest = two(rad_ref[...])
        middle, low = two(rest)
        col = col_ref[...]
        code = (col // LOW) * ROWS_DEV + rib_ref[...] + 1
        payload = jnp.concatenate(
            [high, middle, low]
            + [code.astype(F32), (col & (LOW - 1)).astype(F32)]
            + [jnp.zeros((PACK - 3 * fields - 2, obs), F32)],
            axis=0,
        ).astype(BF16)
        zero = jnp.zeros((PACK, LANES), BF16)
        left = []
        for k in range(obs // LANES):
            load = payload[:, k * LANES : (k + 1) * LANES]
            left.append(
                jnp.concatenate(
                    [
                        jnp.where(keys[k] == jnp.full((PACK, LANES), key, BF16), load, zero)
                        for key in range(nrows * parts)
                    ],
                    axis=0,
                )
            )
        product(accs, [list(x) for x in zip(left, hots)], True)
        placed = pltpu.matmul_pop(accs[0]) + pltpu.matmul_pop(accs[1])
        for d in far + [0]:
            target = sent if d > 0 else arrived
            for p in range(parts):
                part = placed[(d * parts + p) * PACK : (d * parts + p + 1) * PACK]
                values = (part[:fields] + part[fields : 2 * fields]) + part[2 * fields : 3 * fields]
                cells = part[3 * fields : 3 * fields + 1] * LOW + part[3 * fields + 1 : 3 * fields + 2]
                for i in range(wide // LANES):
                    t = p * (wide // LANES) + i
                    span = slice(i * LANES, (i + 1) * LANES)
                    at = (d * lines + t) * 8
                    staged[at : at + fields] = values[:, span]
                    staged[at + fields : at + fields + 1] = cells[:, span]
            for f in range(fields + 1):
                target[d, f] = staged[pl.ds(d * lines * 8 + f, lines, stride=8), :]
        return rank

    rows_placed = nrows * max(1, cap // LOW) * PACK
    rank = pl.run_scoped(
        place_all,
        pltpu.ACC(0)((nrows * obs // LOW, LOW), F32),
        pltpu.ACC(0)((rows_placed, LOW), F32),
        pltpu.ACC(1)((rows_placed, LOW), F32),
    )
    pl.semaphore_wait(barrier, nrows + nchan - 2)
    for d in far:
        remote(
            sent.at[d], arrived.at[d], 0, came.at[d // half_rows + (d + 1) // nrows], rows=row_peer[d]
        ).start()
    for e in range(1, nchan):
        pl.semaphore_signal(ready, inc=1, device_id={"chan": flip(mc, e)}, device_id_type=MESH)


    def cells_all(acc_0, acc_1, *looks):
        accs = (acc_0, acc_1)
        groups = [[0], list(range(1, half_rows)), list(range(half_rows, nrows - 1)), [nrows - 1]]
        for slots in groups:
            if slots[0] > 0:
                at = slots[0] // half_rows + (slots[0] + 1) // nrows
                wait_all(arrived.at[slots[0] : slots[-1] + 1], came.at[at])
            product(accs, tiles_of(arrived, col_hot, slots), True)

        total = pltpu.matmul_pop(accs[0]) + pltpu.matmul_pop(accs[1])
        count, firsts, seconds = grids_of(total, fields)
        inverse = 1.0 / jnp.maximum(count, 1.0)
        partial = None
        means, variances = [], []
        for f in range(fields):
            mean = firsts[f] * inverse
            variance = jnp.maximum(seconds[f] * inverse - mean * mean, 0.0)
            means.append(mean)
            variances.append(variance)
            partial = variance if partial is None else partial + variance

        split = [two(x) for x in means + [partial]]
        pad = jnp.zeros((-(fields + 1) * QS % PACK, LOW), F32)
        table = [jnp.concatenate([x[k] for x in split] + [pad], axis=0).astype(BF16) for k in (0, 1)]
        places = [(d, t) for d in far + [0] for t in range(lines)]
        tiles = [places[i : i + 2] for i in range(0, len(places), 2)]

        def issue(i):
            register = i // 2 % 2
            hot = jnp.concatenate(
                [col_hot[d, :, t * LANES : (t + 1) * LANES] for d, t in tiles[i]], axis=1
            )
            acc = looks[i % len(looks)]
            pltpu.matmul_push_rhs(hot, staging_register=register, mxu_index=i % 2)
            pltpu.matmul_acc_lhs(acc, table[0], load_staged_rhs=register)
            pltpu.matmul_acc_lhs(acc, table[1])

        pl.semaphore_wait(ready, nchan - 1)
        for i in range(min(len(looks), len(tiles))):
            issue(i)
        for i, tile in enumerate(tiles):
            picked = pltpu.matmul_pop(looks[i % len(looks)])
            if i + len(looks) < len(tiles):
                issue(i + len(looks))
            for k, (d, t) in enumerate(tile):
                span = slice(k * LANES, (k + 1) * LANES)
                target = back_s if d > 0 else back_r
                high = arrived[d, fields, t : t + 1].astype(jnp.int32) // LOW - 1
                here = iota((QS, LANES), 0) == high
                for f in range(fields + 1):
                    both = picked[f * QS : (f + 1) * QS, span]
                    found = jnp.sum(jnp.where(here, both, 0.0), axis=0, keepdims=True)
                    if f < fields:
                        target[d, f, t : t + 1] = arrived[d, f, t : t + 1] - found
                    else:
                        target[d, f, t : t + 1] = found
                if t < lines - 1:
                    continue
                for e in range(nchan - 1, 0, -1):
                    slot = e * nrows + d
                    remote(
                        target.at[d, fields],
                        scale_r.at[slot],
                        2,
                        scales.at[d // half_rows],
                        rows=row_peer[d],
                        chan=flip(mc, e),
                    ).start()
                if d > 0:
                    remote(
                        back_s.at[d], back_r.at[d], 1, back.at[d // half_rows], rows=row_peer[d]
                    ).start()
        part_s[...] = partial
        part_copy = remote(part_s, part_r, 3, shares.at[0], chan=partner)
        part_copy.start()

        spill(cnt_out, count)
        for f in range(fields):
            spill(mean_out.at[f], means[f])
            spill(var_out.at[f], variances[f])
        part_copy.wait_recv()
        mine = mc // 2
        pairs[mine] = part_s[...] + part_r[...]
        for j in range(1, npair):
            remote(pairs.at[mine], pairs.at[mine], 4, shares.at[1], chan=chan_peer[j]).start()

        place = jnp.bitwise_xor(folded(dest), me) * lines + rank // LANES
        lane = rank & (LANES - 1)
        found = [jnp.zeros(rank.shape, F32) for _ in range(fields + 1)]
        far_half = list(range(nrows - 1, half_rows - 1, -1))
        returns = [list(range(half_rows)), far_half]
        for slots in returns:
            first = max(1, min(slots))
            wait_all(back_r.at[first : max(slots) + 1], back.at[first // half_rows])
            for d in slots:
                for t in range(lines):
                    here = place == d * lines + t
                    for f in range(fields):
                        found[f] = jnp.where(here, take(back_r[d, f, t : t + 1], lane), found[f])
        wait_all(pairs.at[1:], shares.at[1])
        spread = pairs[0]
        for p in range(1, npair):
            spread = spread + pairs[p]
        spill(spr_out, spread)
        wait_all(sent.at[1:], send.at[0])
        wait_all(back_s.at[1:], send.at[1])
        wait_all(scale_r.at[nrows:], send.at[2])
        part_copy.wait_send()
        wait_all(pairs.at[1:], send.at[4])
        for slots in returns:
            wait_all(
                scale_r.at[nrows : nrows + (nchan - 1) * len(slots)],
                scales.at[slots[0] // half_rows],
            )
            for d in slots:
                for t in range(lines):
                    here = place == d * lines + t
                    row = back_r[d, fields, t : t + 1]
                    for e in range(1, nchan):
                        row = row + scale_r[e * nrows + d, t : t + 1]
                    found[fields] = jnp.where(here, take(row, lane), found[fields])
        scale = lax.rsqrt(1.0 + found[fields] / CHAN)
        many = obs // LANES
        for f in range(fields):
            turned[f * many : (f + 1) * many] = found[f] * scale
        for k in range(many):
            dep_out[:, k * LANES : (k + 1) * LANES] = turned[pl.ds(k, fields, stride=many), :]

    rows_summed = QS * 4 * fields + -(-QS // PACK) * PACK
    rows_looked = -(-(fields + 1) * QS // PACK) * PACK
    pl.run_scoped(
        cells_all,
        *(pltpu.ACC(unit)((rows_summed, LOW), F32) for unit in (0, 1)),
        *(pltpu.ACC(unit)((rows_looked, LOW), F32) for unit in (0, 1) * 4),
    )


def finish(*refs):
    half = (len(refs) - 1) // 2
    sems = refs[-1]
    copies = [
        pltpu.make_async_copy(a, b, sems.at[i])
        for i, (a, b) in enumerate(zip(refs[:half], refs[half : 2 * half]))
    ]
    for copy in copies:
        copy.start()
    for copy in copies:
        copy.wait()


def body(radiances, band, row_in_band, column):
    nrows = lax.axis_size("rows")
    nchan = lax.axis_size("chan")
    fields, obs = radiances.shape
    cap = 2 * obs // nrows
    lines = cap // LANES
    npair = nchan // 2
    vmem = pl.BlockSpec(memory_space=pltpu.VMEM)
    anywhere = pl.BlockSpec(memory_space=pl.ANY)
    dma = pltpu.SemaphoreType.DMA
    shapes = (
        ((ROWS_DEV, COLS), jnp.int32),
        ((fields, ROWS_DEV, COLS), F32),
        ((fields, ROWS_DEV, COLS), F32),
        ((ROWS_DEV, COLS), F32),
        ((fields, obs), F32),
    )
    held = pl.pallas_call(
        functools.partial(kernel, nrows, nchan),
        out_shape=tuple(pltpu.VMEM(s, t) for s, t in shapes),
        in_specs=[pl.BlockSpec(memory_space=pltpu.HBM)] * 4,
        out_specs=(vmem,) * len(shapes),
        scratch_shapes=[
            pltpu.VMEM((fields, obs), F32),
            pltpu.VMEM((1, obs), jnp.int32),
            pltpu.VMEM((1, obs), jnp.int32),
            pltpu.VMEM((1, obs), jnp.int32),
            pltpu.VMEM((nrows * lines * 8, LANES), F32),
            pltpu.VMEM((nrows, fields + 1, lines, LANES), F32),
            pltpu.VMEM((nrows, fields + 1, lines, LANES), F32),
            pltpu.VMEM((nrows, LOW, cap), BF16),
            pltpu.VMEM((QS, LOW), F32),
            pltpu.VMEM((QS, LOW), F32),
            pltpu.VMEM((npair, QS, LOW), F32),
            pltpu.VMEM((nrows, fields + 1, lines, LANES), F32),
            pltpu.VMEM((nrows, fields + 1, lines, LANES), F32),
            pltpu.VMEM((nchan * nrows, lines, LANES), F32),
            pltpu.VMEM((fields * obs // LANES, LANES), F32),
            pltpu.SemaphoreType.REGULAR,
            dma((4,)),
            dma((5,)),
            dma((3,)),
            dma((2,)),
            dma((2,)),
            dma((2,)),
        ],
        compiler_params=pltpu.CompilerParams(
            collective_id=0, has_side_effects=True, vmem_limit_bytes=32 * 1024 * 1024
        ),
    )(
        *(
            pltpu.with_memory_space_constraint(x, pltpu.HBM)
            for x in (
                radiances,
                band.reshape(1, obs),
                row_in_band.reshape(1, obs),
                column.reshape(1, obs),
            )
        )
    )
    return pl.pallas_call(
        finish,
        out_shape=tuple(jax.ShapeDtypeStruct(s, t) for s, t in shapes),
        in_specs=[vmem] * len(shapes),
        out_specs=(anywhere,) * len(shapes),
        scratch_shapes=[dma((len(shapes),))],
        compiler_params=pltpu.CompilerParams(vmem_limit_bytes=32 * 1024 * 1024),
    )(*held)


def solution(mesh):
    in_specs = (P("chan", "rows"), P("rows", None), P("rows"), P("rows"))
    out_specs = (
        P("rows", None),
        P("chan", "rows", None),
        P("chan", "rows", None),
        P("rows", None),
        P("chan", "rows"),
    )
    return jax.shard_map(body, mesh=mesh, in_specs=in_specs, out_specs=out_specs, check_vma=False)
```

```python
import functools

import jax
import jax.numpy as jnp
from jax import lax
from jax.experimental import pallas as pl
from jax.experimental.pallas import tpu as pltpu
from jax.sharding import PartitionSpec as P

CHAN = 16
PACK = 16
COLS = 1440
ROWS_DEV = 4
LOW = 256
LANES = 128
BLOCKS = -(-COLS // LOW)
QS = BLOCKS * ROWS_DEV
F32 = jnp.float32
BF16 = jnp.bfloat16
MESH = pl.DeviceIdType.MESH
NT = (((1,), (1,)), ((), ()))
NN = (((1,), (0,)), ((), ()))


def iota(shape, axis):
    return lax.broadcasted_iota(jnp.int32, shape, axis)


def onehot(mask):
    return jnp.where(mask, 1.0, 0.0)


def two(values):
    high = values.astype(BF16).astype(F32)
    return high, values - high


def product(accs, tiles, transpose):
    for i in range(0, len(tiles), 2):
        pair = tiles[i : i + 2]
        if len(pair) < 2:
            pair.append([jnp.zeros_like(x) for x in pair[0]])
        left, right = (jnp.concatenate(x, axis=1) for x in zip(*pair))
        unit, register = i // 2 % 2, i // 4 % 2
        pltpu.matmul_push_rhs(
            right, staging_register=register, mxu_index=unit, transpose=transpose
        )
        pltpu.matmul_acc_lhs(accs[unit], left, load_staged_rhs=register)


def flip(index, bits):
    out, bit = index, 1
    while bit <= bits:
        if bits & bit:
            out = out + bit - 2 * bit * ((index // bit) % 2)
        bit *= 2
    return out


def rank_of(dest, nrows, acc):
    obs = dest.shape[1]
    nblock = obs // LOW
    hot = [
        onehot(iota((nrows, LOW), 0) == dest[:, b * LOW : (b + 1) * LOW]) for b in range(nblock)
    ]
    upper = onehot(iota((LOW, LOW), 0) < iota((LOW, LOW), 1)).astype(BF16)
    pltpu.matmul_push_rhs(upper, staging_register=0, mxu_index=0)
    pltpu.matmul_acc_lhs(acc, jnp.concatenate(hot, axis=0).astype(BF16), load_staged_rhs=0)
    inner = pltpu.matmul_pop(acc)
    rows, before = [], None
    for b in range(nblock):
        count = inner[b * nrows : (b + 1) * nrows]
        if before is not None:
            count = count + before
        row = jnp.sum(hot[b] * count, axis=0, keepdims=True)
        rows += [row[:, k : k + LANES] for k in range(0, LOW, LANES)]
        size = jnp.sum(hot[b], axis=1, keepdims=True)
        before = size if before is None else before + size
    return rows


def spill(out, values):
    for j in range(BLOCKS):
        start = j * LOW
        width = min(LOW, COLS - start)
        out[:, start : start + width] = values[j * ROWS_DEV : (j + 1) * ROWS_DEV, :width].astype(
            out.dtype
        )


def folded(row):
    lines = row.shape[1] // LANES
    return jnp.concatenate([row[:, k * LANES : (k + 1) * LANES] for k in range(lines)], axis=0)


def take(row, lane):
    return jnp.take_along_axis(
        jnp.broadcast_to(row, lane.shape), lane, axis=1, mode="promise_in_bounds"
    )


def packed(row):
    return jnp.broadcast_to(row, (PACK, row.shape[1])).astype(BF16)


def steps(first, period=PACK):
    return (iota((PACK, LANES), 0) % period + first).astype(F32).astype(BF16)


def low_hot(row, size):
    wide = packed(row)
    one, zero = jnp.ones((PACK, LANES), BF16), jnp.zeros((PACK, LANES), BF16)
    return jnp.concatenate(
        [jnp.where(steps(b) == wide, one, zero) for b in range(0, size, PACK)], axis=0
    )


def tiles_of(arrived, col_hot, slots):
    fields, lines = arrived.shape[1] - 1, arrived.shape[2]
    one, zero = jnp.ones((PACK, LANES), BF16), jnp.zeros((PACK, LANES), BF16)
    tiles = []
    for d in slots:
        cells = arrived[d, fields]
        high = jnp.floor(cells * (1.0 / LOW))
        low, high = cells - high * LOW, high - 1.0
        features = []
        for f in range(fields):
            x = arrived[d, f]
            features += [two(x), two(x * x)]
        for t in range(lines):
            hot = low_hot(low[t : t + 1], LOW)
            col_hot[d, :, t * LANES : (t + 1) * LANES] = hot
            quad = packed(high[t : t + 1])
            pairs = [
                jnp.concatenate(
                    [jnp.broadcast_to(x[t : t + 1], (8, LANES)) for x in feature], axis=0
                ).astype(BF16)
                for feature in features
            ]
            rows = []
            for j in range(0, QS, 8):
                here = steps(j, 8) == quad
                rows += [jnp.where(here, x, zero) for x in pairs]
            for j in range(0, QS, PACK):
                rows.append(jnp.where(steps(j) == quad, one, zero))
            tiles.append([jnp.concatenate(rows, axis=0), hot])
    return tiles


def grids_of(total, fields):
    out = []
    for p in range(2 * fields):
        rows = []
        for j in range(QS // 8):
            at = (j * 2 * fields + p) * 16
            rows.append(total[at : at + 8] + total[at + 8 : at + 16])
        out.append(jnp.concatenate(rows, axis=0))
    at = QS // 8 * 2 * fields * 16
    return total[at : at + QS], out[0::2], out[1::2]


def kernel(
    nrows,
    nchan,
    rad_in,
    band_in,
    rib_in,
    col_in,
    cnt_out,
    mean_out,
    var_out,
    spr_out,
    dep_out,
    rad_ref,
    band_ref,
    rib_ref,
    col_ref,
    staged,
    sent,
    arrived,
    col_hot,
    part_s,
    part_r,
    pairs,
    back_s,
    back_r,
    scale_r,
    turned,
    ready,
    ins,
    send,
    came,
    back,
    scales,
    shares,
):
    me = lax.axis_index("rows")
    mc = lax.axis_index("chan")
    fields, obs = rad_ref.shape
    cap = 2 * obs // nrows
    lines = cap // LANES
    npair = nchan // 2
    half_rows = nrows // 2
    far = sorted(range(1, nrows), key=lambda d: (d // half_rows, d % 2, d), reverse=True)
    row_peer = [flip(me, d) for d in range(nrows)]
    chan_peer = [lax.rem(mc + 2 * j, nchan) for j in range(npair)]
    partner = flip(mc, 1)

    def wait_all(ref, semaphore):
        pltpu.make_async_copy(ref, ref, semaphore).wait()

    def remote(src, dst, recv, **to):
        return pltpu.make_async_remote_copy(
            src_ref=src,
            dst_ref=dst,
            send_sem=send.at[0],
            recv_sem=recv,
            device_id=to,
            device_id_type=MESH,
        )

    barrier = pltpu.get_barrier_semaphore()
    for d in far:
        pl.semaphore_signal(
            barrier, inc=1, device_id={"rows": row_peer[d]}, device_id_type=MESH
        )
    for e in range(1, nchan):
        pl.semaphore_signal(barrier, inc=1, device_id={"chan": flip(mc, e)}, device_id_type=MESH)
    fetches = [
        pltpu.make_async_copy(a, b, ins.at[min(i, 1)])
        for i, (a, b) in enumerate(
            ((band_in, band_ref), (rad_in, rad_ref), (rib_in, rib_ref), (col_in, col_ref))
        )
    ]
    for fetch in fetches:
        fetch.start()

    fetches[0].wait()
    dest = band_ref[...]

    def place_all(acc_rank, *accs):
        ranks = rank_of(dest, nrows, acc_rank)
        rank = folded(jnp.concatenate(ranks, axis=1)).astype(jnp.int32)
        wide = min(cap, LOW)
        parts = cap // wide
        hots, keys = [], []
        for k in range(obs // LANES):
            upper = jnp.floor(ranks[k] * (1.0 / wide))
            hots.append(low_hot(ranks[k] - upper * wide, LOW))
            names = jnp.bitwise_xor(dest[:, k * LANES : (k + 1) * LANES], me)
            keys.append(packed(names.astype(F32) * parts + upper))
        wait_all(staged.at[: (fields + 2) * obs // LANES], ins.at[1])
        high, rest = two(rad_ref[...])
        middle, low = two(rest)
        col = col_ref[...]
        code = (col // LOW) * ROWS_DEV + rib_ref[...] + 1
        payload = jnp.concatenate(
            [high, middle, low]
            + [code.astype(F32), (col & (LOW - 1)).astype(F32)]
            + [jnp.zeros((PACK - 3 * fields - 2, obs), F32)],
            axis=0,
        ).astype(BF16)
        zero = jnp.zeros((PACK, LANES), BF16)
        left = []
        for k in range(obs // LANES):
            load = payload[:, k * LANES : (k + 1) * LANES]
            left.append(
                jnp.concatenate(
                    [
                        jnp.where(keys[k] == jnp.full((PACK, LANES), key, BF16), load, zero)
                        for key in range(nrows * parts)
                    ],
                    axis=0,
                )
            )
        product(accs, [list(x) for x in zip(left, hots)], True)
        placed = pltpu.matmul_pop(accs[0]) + pltpu.matmul_pop(accs[1])
        for d in far + [0]:
            target = sent if d > 0 else arrived
            for p in range(parts):
                part = placed[(d * parts + p) * PACK : (d * parts + p + 1) * PACK]
                values = (part[:fields] + part[fields : 2 * fields]) + part[2 * fields : 3 * fields]
                cells = part[3 * fields : 3 * fields + 1] * LOW + part[3 * fields + 1 : 3 * fields + 2]
                for i in range(wide // LANES):
                    t = p * (wide // LANES) + i
                    span = slice(i * LANES, (i + 1) * LANES)
                    at = (d * lines + t) * 8
                    staged[at : at + fields] = values[:, span]
                    staged[at + fields : at + fields + 1] = cells[:, span]
            for f in range(fields + 1):
                target[d, f] = staged[pl.ds(d * lines * 8 + f, lines, stride=8), :]
        return rank

    rows_placed = nrows * max(1, cap // LOW) * PACK
    rank = pl.run_scoped(
        place_all,
        pltpu.ACC(0)((nrows * obs // LOW, LOW), F32),
        pltpu.ACC(0)((rows_placed, LOW), F32),
        pltpu.ACC(1)((rows_placed, LOW), F32),
    )
    pl.semaphore_wait(barrier, nrows + nchan - 2)
    for d in far:
        remote(
            sent.at[d], arrived.at[d], came.at[d // half_rows + (d + 1) // nrows], rows=row_peer[d]
        ).start()
    for e in range(1, nchan):
        pl.semaphore_signal(ready, inc=1, device_id={"chan": flip(mc, e)}, device_id_type=MESH)


    def cells_all(acc_0, acc_1, *looks):
        accs = (acc_0, acc_1)
        groups = [[0], list(range(1, half_rows)), list(range(half_rows, nrows - 1)), [nrows - 1]]
        for slots in groups:
            if slots[0] == nrows - 1:
                wait_all(sent.at[1:], send.at[0])
                pl.semaphore_wait(ready, nchan - 1)
            if slots[0] > 0:
                at = slots[0] // half_rows + (slots[0] + 1) // nrows
                wait_all(arrived.at[slots[0] : slots[-1] + 1], came.at[at])
            product(accs, tiles_of(arrived, col_hot, slots), True)

        total = pltpu.matmul_pop(accs[0]) + pltpu.matmul_pop(accs[1])
        count, firsts, seconds = grids_of(total, fields)
        inverse = 1.0 / jnp.maximum(count, 1.0)
        partial = None
        means, variances = [], []
        for f in range(fields):
            mean = firsts[f] * inverse
            variance = jnp.maximum(seconds[f] * inverse - mean * mean, 0.0)
            means.append(mean)
            variances.append(variance)
            partial = variance if partial is None else partial + variance

        split = [two(x) for x in means + [partial]]
        pad = jnp.zeros((-(fields + 1) * QS % PACK, LOW), F32)
        table = [jnp.concatenate([x[k] for x in split] + [pad], axis=0).astype(BF16) for k in (0, 1)]
        places = [(d, t) for d in far + [0] for t in range(lines)]
        tiles = [places[i : i + 2] for i in range(0, len(places), 2)]

        def issue(i):
            register = i // 2 % 2
            hot = jnp.concatenate(
                [col_hot[d, :, t * LANES : (t + 1) * LANES] for d, t in tiles[i]], axis=1
            )
            acc = looks[i % len(looks)]
            pltpu.matmul_push_rhs(hot, staging_register=register, mxu_index=i % 2)
            pltpu.matmul_acc_lhs(acc, table[0], load_staged_rhs=register)
            pltpu.matmul_acc_lhs(acc, table[1])

        for i in range(min(len(looks), len(tiles))):
            issue(i)
        for i, tile in enumerate(tiles):
            picked = pltpu.matmul_pop(looks[i % len(looks)])
            if i + len(looks) < len(tiles):
                issue(i + len(looks))
            for k, (d, t) in enumerate(tile):
                span = slice(k * LANES, (k + 1) * LANES)
                target = back_s if d > 0 else back_r
                high = arrived[d, fields, t : t + 1].astype(jnp.int32) // LOW - 1
                here = iota((QS, LANES), 0) == high
                for f in range(fields + 1):
                    both = picked[f * QS : (f + 1) * QS, span]
                    found = jnp.sum(jnp.where(here, both, 0.0), axis=0, keepdims=True)
                    if f < fields:
                        target[d, f, t : t + 1] = arrived[d, f, t : t + 1] - found
                    else:
                        target[d, f, t : t + 1] = found
                if t < lines - 1:
                    continue
                for e in range(nchan - 1, 0, -1):
                    slot = e * nrows + d
                    remote(
                        target.at[d, fields],
                        scale_r.at[slot],
                        scales.at[d // half_rows],
                        rows=row_peer[d],
                        chan=flip(mc, e),
                    ).start()
                if d > 0:
                    remote(
                        back_s.at[d], back_r.at[d], back.at[d // half_rows], rows=row_peer[d]
                    ).start()
        part_s[...] = partial
        part_copy = remote(part_s, part_r, shares.at[0], chan=partner)
        part_copy.start()

        spill(cnt_out, count)
        for f in range(fields):
            spill(mean_out.at[f], means[f])
            spill(var_out.at[f], variances[f])
        part_copy.wait_recv()
        mine = mc // 2
        pairs[mine] = part_s[...] + part_r[...]
        for j in range(1, npair):
            remote(pairs.at[mine], pairs.at[mine], shares.at[1], chan=chan_peer[j]).start()

        place = jnp.bitwise_xor(folded(dest), me) * lines + rank // LANES
        lane = rank & (LANES - 1)
        found = [jnp.zeros(rank.shape, F32) for _ in range(fields + 1)]
        far_half = list(range(nrows - 1, half_rows - 1, -1))
        returns = [list(range(half_rows)), far_half]
        for slots in returns:
            first = max(1, min(slots))
            wait_all(back_r.at[first : max(slots) + 1], back.at[first // half_rows])
            for d in slots:
                for t in range(lines):
                    here = place == d * lines + t
                    for f in range(fields):
                        found[f] = jnp.where(here, take(back_r[d, f, t : t + 1], lane), found[f])
        wait_all(pairs.at[1:], shares.at[1])
        spread = pairs[0]
        for p in range(1, npair):
            spread = spread + pairs[p]
        spill(spr_out, spread)
        lent = (nrows - 1) * (fields + 1) + (nchan - 1) * nrows
        wait_all(staged.at[: lent * lines + npair * QS * LOW // LANES], send.at[0])
        for slots in returns:
            wait_all(
                scale_r.at[nrows : nrows + (nchan - 1) * len(slots)],
                scales.at[slots[0] // half_rows],
            )
            for d in slots:
                for t in range(lines):
                    here = place == d * lines + t
                    row = back_r[d, fields, t : t + 1]
                    for e in range(1, nchan):
                        row = row + scale_r[e * nrows + d, t : t + 1]
                    found[fields] = jnp.where(here, take(row, lane), found[fields])
        scale = lax.rsqrt(1.0 + found[fields] / CHAN)
        many = obs // LANES
        for f in range(fields):
            turned[f * many : (f + 1) * many] = found[f] * scale
        for k in range(many):
            dep_out[:, k * LANES : (k + 1) * LANES] = turned[pl.ds(k, fields, stride=many), :]

    rows_summed = QS * 4 * fields + -(-QS // PACK) * PACK
    rows_looked = -(-(fields + 1) * QS // PACK) * PACK
    pl.run_scoped(
        cells_all,
        *(pltpu.ACC(unit)((rows_summed, LOW), F32) for unit in (0, 1)),
        *(pltpu.ACC(unit)((rows_looked, LOW), F32) for unit in (0, 1) * 4),
    )


def finish(*refs):
    half = (len(refs) - 1) // 2
    sems = refs[-1]
    copies = [
        pltpu.make_async_copy(a, b, sems.at[i])
        for i, (a, b) in enumerate(zip(refs[:half], refs[half : 2 * half]))
    ]
    for copy in copies:
        copy.start()
    for copy in copies:
        copy.wait()


def body(radiances, band, row_in_band, column):
    nrows = lax.axis_size("rows")
    nchan = lax.axis_size("chan")
    fields, obs = radiances.shape
    cap = 2 * obs // nrows
    lines = cap // LANES
    npair = nchan // 2
    vmem = pl.BlockSpec(memory_space=pltpu.VMEM)
    anywhere = pl.BlockSpec(memory_space=pl.ANY)
    dma = pltpu.SemaphoreType.DMA
    shapes = (
        ((ROWS_DEV, COLS), jnp.int32),
        ((fields, ROWS_DEV, COLS), F32),
        ((fields, ROWS_DEV, COLS), F32),
        ((ROWS_DEV, COLS), F32),
        ((fields, obs), F32),
    )
    held = pl.pallas_call(
        functools.partial(kernel, nrows, nchan),
        out_shape=tuple(pltpu.VMEM(s, t) for s, t in shapes),
        in_specs=[pl.BlockSpec(memory_space=pltpu.HBM)] * 4,
        out_specs=(vmem,) * len(shapes),
        scratch_shapes=[
            pltpu.VMEM((fields, obs), F32),
            pltpu.VMEM((1, obs), jnp.int32),
            pltpu.VMEM((1, obs), jnp.int32),
            pltpu.VMEM((1, obs), jnp.int32),
            pltpu.VMEM((nrows * lines * 16, LANES), F32),
            pltpu.VMEM((nrows, fields + 1, lines, LANES), F32),
            pltpu.VMEM((nrows, fields + 1, lines, LANES), F32),
            pltpu.VMEM((nrows, LOW, cap), BF16),
            pltpu.VMEM((QS, LOW), F32),
            pltpu.VMEM((QS, LOW), F32),
            pltpu.VMEM((npair, QS, LOW), F32),
            pltpu.VMEM((nrows, fields + 1, lines, LANES), F32),
            pltpu.VMEM((nrows, fields + 1, lines, LANES), F32),
            pltpu.VMEM((nchan * nrows, lines, LANES), F32),
            pltpu.VMEM((fields * obs // LANES, LANES), F32),
            pltpu.SemaphoreType.REGULAR,
            dma((2,)),
            dma((1,)),
            dma((3,)),
            dma((2,)),
            dma((2,)),
            dma((2,)),
        ],
        compiler_params=pltpu.CompilerParams(
            collective_id=0, has_side_effects=True, vmem_limit_bytes=32 * 1024 * 1024
        ),
    )(
        *(
            pltpu.with_memory_space_constraint(x, pltpu.HBM)
            for x in (
                radiances,
                band.reshape(1, obs),
                row_in_band.reshape(1, obs),
                column.reshape(1, obs),
            )
        )
    )
    return pl.pallas_call(
        finish,
        out_shape=tuple(jax.ShapeDtypeStruct(s, t) for s, t in shapes),
        in_specs=[vmem] * len(shapes),
        out_specs=(anywhere,) * len(shapes),
        scratch_shapes=[dma((len(shapes),))],
        compiler_params=pltpu.CompilerParams(vmem_limit_bytes=32 * 1024 * 1024),
    )(*held)


def solution(mesh):
    in_specs = (P("chan", "rows"), P("rows", None), P("rows"), P("rows"))
    out_specs = (
        P("rows", None),
        P("chan", "rows", None),
        P("chan", "rows", None),
        P("rows", None),
        P("chan", "rows"),
    )
    return jax.shard_map(body, mesh=mesh, in_specs=in_specs, out_specs=out_specs, check_vma=False)
```

```python
import functools

import jax
import jax.numpy as jnp
from jax import lax
from jax.experimental import pallas as pl
from jax.experimental.pallas import tpu as pltpu
from jax.sharding import PartitionSpec as P

CHAN = 16
PACK = 16
COLS = 1440
ROWS_DEV = 4
LOW = 256
LANES = 128
BLOCKS = -(-COLS // LOW)
QS = BLOCKS * ROWS_DEV
F32 = jnp.float32
BF16 = jnp.bfloat16
MESH = pl.DeviceIdType.MESH
NT = (((1,), (1,)), ((), ()))
NN = (((1,), (0,)), ((), ()))


def iota(shape, axis):
    return lax.broadcasted_iota(jnp.int32, shape, axis)


def onehot(mask):
    return jnp.where(mask, 1.0, 0.0)


def two(values):
    high = values.astype(BF16).astype(F32)
    return high, values - high


def product(accs, tiles, transpose):
    for i in range(0, len(tiles), 2):
        pair = tiles[i : i + 2]
        if len(pair) < 2:
            pair.append([jnp.zeros_like(x) for x in pair[0]])
        left, right = (jnp.concatenate(x, axis=1) for x in zip(*pair))
        unit, register = i // 2 % 2, i // 4 % 2
        pltpu.matmul_push_rhs(
            right, staging_register=register, mxu_index=unit, transpose=transpose
        )
        pltpu.matmul_acc_lhs(accs[unit], left, load_staged_rhs=register)


def flip(index, bits):
    out, bit = index, 1
    while bit <= bits:
        if bits & bit:
            out = out + bit - 2 * bit * ((index // bit) % 2)
        bit *= 2
    return out


def rank_of(dest, nrows, acc):
    obs = dest.shape[1]
    nblock = obs // LOW
    hot = [
        onehot(iota((nrows, LOW), 0) == dest[:, b * LOW : (b + 1) * LOW]) for b in range(nblock)
    ]
    upper = onehot(iota((LOW, LOW), 0) < iota((LOW, LOW), 1)).astype(BF16)
    pltpu.matmul_push_rhs(upper, staging_register=0, mxu_index=0)
    pltpu.matmul_acc_lhs(acc, jnp.concatenate(hot, axis=0).astype(BF16), load_staged_rhs=0)
    inner = pltpu.matmul_pop(acc)
    rows, before = [], None
    for b in range(nblock):
        count = inner[b * nrows : (b + 1) * nrows]
        if before is not None:
            count = count + before
        row = jnp.sum(hot[b] * count, axis=0, keepdims=True)
        rows += [row[:, k : k + LANES] for k in range(0, LOW, LANES)]
        size = jnp.sum(hot[b], axis=1, keepdims=True)
        before = size if before is None else before + size
    return rows


def spill(out, values):
    for j in range(BLOCKS):
        start = j * LOW
        width = min(LOW, COLS - start)
        out[:, start : start + width] = values[j * ROWS_DEV : (j + 1) * ROWS_DEV, :width].astype(
            out.dtype
        )


def folded(row):
    lines = row.shape[1] // LANES
    return jnp.concatenate([row[:, k * LANES : (k + 1) * LANES] for k in range(lines)], axis=0)


def take(row, lane):
    return jnp.take_along_axis(
        jnp.broadcast_to(row, lane.shape), lane, axis=1, mode="promise_in_bounds"
    )


def packed(row):
    return jnp.broadcast_to(row, (PACK, row.shape[1])).astype(BF16)


def steps(first, period=PACK):
    return (iota((PACK, LANES), 0) % period + first).astype(F32).astype(BF16)


def low_hot(row, size):
    wide = packed(row)
    one, zero = jnp.ones((PACK, LANES), BF16), jnp.zeros((PACK, LANES), BF16)
    return jnp.concatenate(
        [jnp.where(steps(b) == wide, one, zero) for b in range(0, size, PACK)], axis=0
    )


def tiles_of(arrived, col_hot, slots):
    fields, lines = arrived.shape[1] - 1, arrived.shape[2]
    one, zero = jnp.ones((PACK, LANES), BF16), jnp.zeros((PACK, LANES), BF16)
    tiles = []
    for d in slots:
        cells = arrived[d, fields]
        high = jnp.floor(cells * (1.0 / LOW))
        low, high = cells - high * LOW, high - 1.0
        features = []
        for f in range(fields):
            x = arrived[d, f]
            features += [two(x), two(x * x)]
        for t in range(lines):
            hot = low_hot(low[t : t + 1], LOW)
            col_hot[d, :, t * LANES : (t + 1) * LANES] = hot
            quad = packed(high[t : t + 1])
            pairs = [
                jnp.concatenate(
                    [jnp.broadcast_to(x[t : t + 1], (8, LANES)) for x in feature], axis=0
                ).astype(BF16)
                for feature in features
            ]
            rows = []
            for j in range(0, QS, 8):
                here = steps(j, 8) == quad
                rows += [jnp.where(here, x, zero) for x in pairs]
            for j in range(0, QS, PACK):
                rows.append(jnp.where(steps(j) == quad, one, zero))
            tiles.append([jnp.concatenate(rows, axis=0), hot])
    return tiles


def grids_of(total, fields):
    out = []
    for p in range(2 * fields):
        rows = []
        for j in range(QS // 8):
            at = (j * 2 * fields + p) * 16
            rows.append(total[at : at + 8] + total[at + 8 : at + 16])
        out.append(jnp.concatenate(rows, axis=0))
    at = QS // 8 * 2 * fields * 16
    return total[at : at + QS], out[0::2], out[1::2]


def kernel(
    nrows,
    nchan,
    rad_in,
    band_in,
    rib_in,
    col_in,
    cnt_out,
    mean_out,
    var_out,
    spr_out,
    dep_out,
    rad_ref,
    band_ref,
    rib_ref,
    col_ref,
    staged,
    sent,
    arrived,
    col_hot,
    part_s,
    part_r,
    pairs,
    back_s,
    back_r,
    scale_r,
    turned,
    ledger,
    ready,
    ins,
    send,
    came,
    back,
    scales,
    shares,
):
    me = lax.axis_index("rows")
    mc = lax.axis_index("chan")
    fields, obs = rad_ref.shape
    cap = 2 * obs // nrows
    lines = cap // LANES
    npair = nchan // 2
    half_rows = nrows // 2
    far = sorted(range(1, nrows), key=lambda d: (d // half_rows, d % 2, d), reverse=True)
    row_peer = [flip(me, d) for d in range(nrows)]
    chan_peer = [lax.rem(mc + 2 * j, nchan) for j in range(npair)]
    partner = flip(mc, 1)

    def wait_all(ref, semaphore):
        pltpu.make_async_copy(ref, ref, semaphore).wait()

    def remote(src, dst, recv, kind=0, **to):
        return pltpu.make_async_remote_copy(
            src_ref=src,
            dst_ref=dst,
            send_sem=send.at[kind],
            recv_sem=recv,
            device_id=to,
            device_id_type=MESH,
        )

    barrier = pltpu.get_barrier_semaphore()
    for d in far:
        pl.semaphore_signal(
            barrier, inc=1, device_id={"rows": row_peer[d]}, device_id_type=MESH
        )
    for e in range(1, nchan):
        pl.semaphore_signal(barrier, inc=1, device_id={"chan": flip(mc, e)}, device_id_type=MESH)
    fetches = [
        pltpu.make_async_copy(a, b, ins.at[min(i, 1)])
        for i, (a, b) in enumerate(
            ((band_in, band_ref), (rad_in, rad_ref), (rib_in, rib_ref), (col_in, col_ref))
        )
    ]
    for fetch in fetches:
        fetch.start()

    fetches[0].wait()
    dest = band_ref[...]

    def place_all(acc_rank, *accs):
        ranks = rank_of(dest, nrows, acc_rank)
        rank = folded(jnp.concatenate(ranks, axis=1)).astype(jnp.int32)
        wide = min(cap, LOW)
        parts = cap // wide
        hots, keys = [], []
        for k in range(obs // LANES):
            upper = jnp.floor(ranks[k] * (1.0 / wide))
            hots.append(low_hot(ranks[k] - upper * wide, LOW))
            names = jnp.bitwise_xor(dest[:, k * LANES : (k + 1) * LANES], me)
            keys.append(packed(names.astype(F32) * parts + upper))
        wait_all(staged.at[: (fields + 2) * obs // LANES], ins.at[1])
        high, rest = two(rad_ref[...])
        middle, low = two(rest)
        col = col_ref[...]
        code = (col // LOW) * ROWS_DEV + rib_ref[...] + 1
        payload = jnp.concatenate(
            [high, middle, low]
            + [code.astype(F32), (col & (LOW - 1)).astype(F32)]
            + [jnp.zeros((PACK - 3 * fields - 2, obs), F32)],
            axis=0,
        ).astype(BF16)
        zero = jnp.zeros((PACK, LANES), BF16)
        left = []
        for k in range(obs // LANES):
            load = payload[:, k * LANES : (k + 1) * LANES]
            left.append(
                jnp.concatenate(
                    [
                        jnp.where(keys[k] == jnp.full((PACK, LANES), key, BF16), load, zero)
                        for key in range(nrows * parts)
                    ],
                    axis=0,
                )
            )
        product(accs, [list(x) for x in zip(left, hots)], True)
        placed = pltpu.matmul_pop(accs[0]) + pltpu.matmul_pop(accs[1])
        for d in far + [0]:
            target = sent if d > 0 else arrived
            for p in range(parts):
                part = placed[(d * parts + p) * PACK : (d * parts + p + 1) * PACK]
                values = (part[:fields] + part[fields : 2 * fields]) + part[2 * fields : 3 * fields]
                cells = part[3 * fields : 3 * fields + 1] * LOW + part[3 * fields + 1 : 3 * fields + 2]
                for i in range(wide // LANES):
                    t = p * (wide // LANES) + i
                    span = slice(i * LANES, (i + 1) * LANES)
                    at = (d * lines + t) * 8
                    staged[at : at + fields] = values[:, span]
                    staged[at + fields : at + fields + 1] = cells[:, span]
            for f in range(fields + 1):
                target[d, f] = staged[pl.ds(d * lines * 8 + f, lines, stride=8), :]
        return rank

    rows_placed = nrows * max(1, cap // LOW) * PACK
    rank = pl.run_scoped(
        place_all,
        pltpu.ACC(0)((nrows * obs // LOW, LOW), F32),
        pltpu.ACC(0)((rows_placed, LOW), F32),
        pltpu.ACC(1)((rows_placed, LOW), F32),
    )
    pl.semaphore_wait(barrier, nrows + nchan - 2)
    for d in far:
        remote(
            sent.at[d], arrived.at[d], came.at[d // half_rows + (d + 1) // nrows], rows=row_peer[d]
        ).start()
    for e in range(1, nchan):
        pl.semaphore_signal(ready, inc=1, device_id={"chan": flip(mc, e)}, device_id_type=MESH)


    def cells_all(acc_0, acc_1, *looks):
        accs = (acc_0, acc_1)
        groups = [[0], list(range(1, half_rows)), list(range(half_rows, nrows - 1)), [nrows - 1]]
        for slots in groups:
            if slots[0] == nrows - 1:
                wait_all(sent.at[1:], send.at[0])
                pl.semaphore_wait(ready, nchan - 1)
            if slots[0] > 0:
                at = slots[0] // half_rows + (slots[0] + 1) // nrows
                wait_all(arrived.at[slots[0] : slots[-1] + 1], came.at[at])
            product(accs, tiles_of(arrived, col_hot, slots), True)

        total = pltpu.matmul_pop(accs[0]) + pltpu.matmul_pop(accs[1])
        count, firsts, seconds = grids_of(total, fields)
        inverse = 1.0 / jnp.maximum(count, 1.0)
        partial = None
        means, variances = [], []
        for f in range(fields):
            mean = firsts[f] * inverse
            variance = jnp.maximum(seconds[f] * inverse - mean * mean, 0.0)
            means.append(mean)
            variances.append(variance)
            partial = variance if partial is None else partial + variance

        split = [two(x) for x in means + [partial]]
        pad = jnp.zeros((-(fields + 1) * QS % PACK, LOW), F32)
        table = [jnp.concatenate([x[k] for x in split] + [pad], axis=0).astype(BF16) for k in (0, 1)]
        places = [(d, t) for d in far + [0] for t in range(lines)]
        tiles = [places[i : i + 2] for i in range(0, len(places), 2)]

        def issue(i):
            register = i // 2 % 2
            hot = jnp.concatenate(
                [col_hot[d, :, t * LANES : (t + 1) * LANES] for d, t in tiles[i]], axis=1
            )
            acc = looks[i % len(looks)]
            pltpu.matmul_push_rhs(hot, staging_register=register, mxu_index=i % 2)
            pltpu.matmul_acc_lhs(acc, table[0], load_staged_rhs=register)
            pltpu.matmul_acc_lhs(acc, table[1])

        for i in range(min(len(looks), len(tiles))):
            issue(i)
        for i, tile in enumerate(tiles):
            picked = pltpu.matmul_pop(looks[i % len(looks)])
            if i + len(looks) < len(tiles):
                issue(i + len(looks))
            for k, (d, t) in enumerate(tile):
                span = slice(k * LANES, (k + 1) * LANES)
                target = back_s if d > 0 else back_r
                high = arrived[d, fields, t : t + 1].astype(jnp.int32) // LOW - 1
                here = iota((QS, LANES), 0) == high
                for f in range(fields + 1):
                    both = picked[f * QS : (f + 1) * QS, span]
                    found = jnp.sum(jnp.where(here, both, 0.0), axis=0, keepdims=True)
                    if f < fields:
                        target[d, f, t : t + 1] = arrived[d, f, t : t + 1] - found
                    else:
                        target[d, f, t : t + 1] = found
                if t < lines - 1:
                    continue
                for e in range(nchan - 1, 0, -1):
                    slot = e * nrows + d
                    remote(
                        target.at[d, fields],
                        scale_r.at[slot],
                        scales.at[d // half_rows],
                        rows=row_peer[d],
                        chan=flip(mc, e),
                    ).start()
                if d > 0:
                    remote(
                        back_s.at[d], back_r.at[d], back.at[d // half_rows], rows=row_peer[d]
                    ).start()
        part_s[...] = partial
        part_copy = remote(part_s, part_r, shares.at[0], 1, chan=partner)
        part_copy.start()

        spill(cnt_out, count)
        for f in range(fields):
            spill(mean_out.at[f], means[f])
            spill(var_out.at[f], variances[f])
        part_copy.wait_recv()
        mine = mc // 2
        pairs[mine] = part_s[...] + part_r[...]
        for j in range(1, npair):
            remote(pairs.at[mine], pairs.at[mine], shares.at[1], 1, chan=chan_peer[j]).start()

        place = jnp.bitwise_xor(folded(dest), me) * lines + rank // LANES
        lane = rank & (LANES - 1)
        found = [jnp.zeros(rank.shape, F32) for _ in range(fields + 1)]
        far_half = list(range(nrows - 1, half_rows - 1, -1))
        returns = [list(range(half_rows)), far_half]
        for slots in returns:
            first = max(1, min(slots))
            wait_all(back_r.at[first : max(slots) + 1], back.at[first // half_rows])
            for d in slots:
                for t in range(lines):
                    here = place == d * lines + t
                    for f in range(fields):
                        found[f] = jnp.where(here, take(back_r[d, f, t : t + 1], lane), found[f])
        wait_all(pairs.at[1:], shares.at[1])
        spread = pairs[0]
        for p in range(1, npair):
            spread = spread + pairs[p]
        spill(spr_out, spread)
        lent = (nrows - 1) * (fields + 1) + (nchan - 1) * nrows
        wait_all(ledger.at[:lent], send.at[0])
        wait_all(pairs, send.at[1])
        for slots in returns:
            wait_all(
                scale_r.at[nrows : nrows + (nchan - 1) * len(slots)],
                scales.at[slots[0] // half_rows],
            )
            for d in slots:
                for t in range(lines):
                    here = place == d * lines + t
                    row = back_r[d, fields, t : t + 1]
                    for e in range(1, nchan):
                        row = row + scale_r[e * nrows + d, t : t + 1]
                    found[fields] = jnp.where(here, take(row, lane), found[fields])
        scale = lax.rsqrt(1.0 + found[fields] / CHAN)
        many = obs // LANES
        for f in range(fields):
            turned[f * many : (f + 1) * many] = found[f] * scale
        for k in range(many):
            dep_out[:, k * LANES : (k + 1) * LANES] = turned[pl.ds(k, fields, stride=many), :]

    rows_summed = QS * 4 * fields + -(-QS // PACK) * PACK
    rows_looked = -(-(fields + 1) * QS // PACK) * PACK
    pl.run_scoped(
        cells_all,
        *(pltpu.ACC(unit)((rows_summed, LOW), F32) for unit in (0, 1)),
        *(pltpu.ACC(unit)((rows_looked, LOW), F32) for unit in (0, 1) * 4),
    )


def finish(*refs):
    half = (len(refs) - 1) // 2
    sems = refs[-1]
    copies = [
        pltpu.make_async_copy(a, b, sems.at[i])
        for i, (a, b) in enumerate(zip(refs[:half], refs[half : 2 * half]))
    ]
    for copy in copies:
        copy.start()
    for copy in copies:
        copy.wait()


def body(radiances, band, row_in_band, column):
    nrows = lax.axis_size("rows")
    nchan = lax.axis_size("chan")
    fields, obs = radiances.shape
    cap = 2 * obs // nrows
    lines = cap // LANES
    npair = nchan // 2
    vmem = pl.BlockSpec(memory_space=pltpu.VMEM)
    anywhere = pl.BlockSpec(memory_space=pl.ANY)
    dma = pltpu.SemaphoreType.DMA
    shapes = (
        ((ROWS_DEV, COLS), jnp.int32),
        ((fields, ROWS_DEV, COLS), F32),
        ((fields, ROWS_DEV, COLS), F32),
        ((ROWS_DEV, COLS), F32),
        ((fields, obs), F32),
    )
    held = pl.pallas_call(
        functools.partial(kernel, nrows, nchan),
        out_shape=tuple(pltpu.VMEM(s, t) for s, t in shapes),
        in_specs=[pl.BlockSpec(memory_space=pltpu.HBM)] * 4,
        out_specs=(vmem,) * len(shapes),
        scratch_shapes=[
            pltpu.VMEM((fields, obs), F32),
            pltpu.VMEM((1, obs), jnp.int32),
            pltpu.VMEM((1, obs), jnp.int32),
            pltpu.VMEM((1, obs), jnp.int32),
            pltpu.VMEM((nrows * lines * 8, LANES), F32),
            pltpu.VMEM((nrows, fields + 1, lines, LANES), F32),
            pltpu.VMEM((nrows, fields + 1, lines, LANES), F32),
            pltpu.VMEM((nrows, LOW, cap), BF16),
            pltpu.VMEM((QS, LOW), F32),
            pltpu.VMEM((QS, LOW), F32),
            pltpu.VMEM((npair, QS, LOW), F32),
            pltpu.VMEM((nrows, fields + 1, lines, LANES), F32),
            pltpu.VMEM((nrows, fields + 1, lines, LANES), F32),
            pltpu.VMEM((nchan * nrows, lines, LANES), F32),
            pltpu.VMEM((fields * obs // LANES, LANES), F32),
            pltpu.VMEM((nrows * (fields + nchan), lines, LANES), F32),
            pltpu.SemaphoreType.REGULAR,
            dma((2,)),
            dma((2,)),
            dma((3,)),
            dma((2,)),
            dma((2,)),
            dma((2,)),
        ],
        compiler_params=pltpu.CompilerParams(
            collective_id=0, has_side_effects=True, vmem_limit_bytes=32 * 1024 * 1024
        ),
    )(
        *(
            pltpu.with_memory_space_constraint(x, pltpu.HBM)
            for x in (
                radiances,
                band.reshape(1, obs),
                row_in_band.reshape(1, obs),
                column.reshape(1, obs),
            )
        )
    )
    return pl.pallas_call(
        finish,
        out_shape=tuple(jax.ShapeDtypeStruct(s, t) for s, t in shapes),
        in_specs=[vmem] * len(shapes),
        out_specs=(anywhere,) * len(shapes),
        scratch_shapes=[dma((len(shapes),))],
        compiler_params=pltpu.CompilerParams(vmem_limit_bytes=32 * 1024 * 1024),
    )(*held)


def solution(mesh):
    in_specs = (P("chan", "rows"), P("rows", None), P("rows"), P("rows"))
    out_specs = (
        P("rows", None),
        P("chan", "rows", None),
        P("chan", "rows", None),
        P("rows", None),
        P("chan", "rows"),
    )
    return jax.shard_map(body, mesh=mesh, in_specs=in_specs, out_specs=out_specs, check_vma=False)
```

```python
import functools

import jax
import jax.numpy as jnp
from jax import lax
from jax.experimental import pallas as pl
from jax.experimental.pallas import tpu as pltpu
from jax.sharding import PartitionSpec as P

CHAN = 16
PACK = 16
COLS = 1440
ROWS_DEV = 4
LOW = 256
LANES = 128
BLOCKS = -(-COLS // LOW)
QS = BLOCKS * ROWS_DEV
F32 = jnp.float32
BF16 = jnp.bfloat16
MESH = pl.DeviceIdType.MESH
NT = (((1,), (1,)), ((), ()))
NN = (((1,), (0,)), ((), ()))


def iota(shape, axis):
    return lax.broadcasted_iota(jnp.int32, shape, axis)


def onehot(mask):
    return jnp.where(mask, 1.0, 0.0)


def two(values):
    high = values.astype(BF16).astype(F32)
    return high, values - high


def product(accs, tiles, transpose):
    for i in range(0, len(tiles), 2):
        pair = tiles[i : i + 2]
        if len(pair) < 2:
            pair.append([jnp.zeros_like(x) for x in pair[0]])
        left, right = (jnp.concatenate(x, axis=1) for x in zip(*pair))
        unit, register = i // 2 % 2, i // 4 % 2
        pltpu.matmul_push_rhs(
            right, staging_register=register, mxu_index=unit, transpose=transpose
        )
        pltpu.matmul_acc_lhs(accs[unit], left, load_staged_rhs=register)


def flip(index, bits):
    out, bit = index, 1
    while bit <= bits:
        if bits & bit:
            out = out + bit - 2 * bit * ((index // bit) % 2)
        bit *= 2
    return out


def rank_of(dest, nrows, acc):
    obs = dest.shape[1]
    nblock = obs // LOW
    hot = [
        onehot(iota((nrows, LOW), 0) == dest[:, b * LOW : (b + 1) * LOW]) for b in range(nblock)
    ]
    upper = onehot(iota((LOW, LOW), 0) < iota((LOW, LOW), 1)).astype(BF16)
    pltpu.matmul_push_rhs(upper, staging_register=0, mxu_index=0)
    pltpu.matmul_acc_lhs(acc, jnp.concatenate(hot, axis=0).astype(BF16), load_staged_rhs=0)
    inner = pltpu.matmul_pop(acc)
    rows, before = [], None
    for b in range(nblock):
        count = inner[b * nrows : (b + 1) * nrows]
        if before is not None:
            count = count + before
        row = jnp.sum(hot[b] * count, axis=0, keepdims=True)
        rows += [row[:, k : k + LANES] for k in range(0, LOW, LANES)]
        size = jnp.sum(hot[b], axis=1, keepdims=True)
        before = size if before is None else before + size
    return rows


def spill(out, values):
    for j in range(BLOCKS):
        start = j * LOW
        width = min(LOW, COLS - start)
        out[:, start : start + width] = values[j * ROWS_DEV : (j + 1) * ROWS_DEV, :width].astype(
            out.dtype
        )


def folded(row):
    lines = row.shape[1] // LANES
    return jnp.concatenate([row[:, k * LANES : (k + 1) * LANES] for k in range(lines)], axis=0)


def take(row, lane):
    return jnp.take_along_axis(
        jnp.broadcast_to(row, lane.shape), lane, axis=1, mode="promise_in_bounds"
    )


def packed(row):
    return jnp.broadcast_to(row, (PACK, row.shape[1])).astype(BF16)


def steps(first, period=PACK):
    return (iota((PACK, LANES), 0) % period + first).astype(F32).astype(BF16)


def low_hot(row, size):
    wide = packed(row)
    one, zero = jnp.ones((PACK, LANES), BF16), jnp.zeros((PACK, LANES), BF16)
    return jnp.concatenate(
        [jnp.where(steps(b) == wide, one, zero) for b in range(0, size, PACK)], axis=0
    )


def tiles_of(arrived, col_hot, slots):
    fields, lines = arrived.shape[1] - 1, arrived.shape[2]
    one, zero = jnp.ones((PACK, LANES), BF16), jnp.zeros((PACK, LANES), BF16)
    tiles = []
    for d in slots:
        cells = arrived[d, fields]
        high = jnp.floor(cells * (1.0 / LOW))
        low, high = cells - high * LOW, high - 1.0
        features = []
        for f in range(fields):
            x = arrived[d, f]
            features += [two(x), two(x * x)]
        for t in range(lines):
            hot = low_hot(low[t : t + 1], LOW)
            col_hot[d, :, t * LANES : (t + 1) * LANES] = hot
            quad = packed(high[t : t + 1])
            pairs = [
                jnp.concatenate(
                    [jnp.broadcast_to(x[t : t + 1], (8, LANES)) for x in feature], axis=0
                ).astype(BF16)
                for feature in features
            ]
            rows = []
            for j in range(0, QS, 8):
                here = steps(j, 8) == quad
                rows += [jnp.where(here, x, zero) for x in pairs]
            for j in range(0, QS, PACK):
                rows.append(jnp.where(steps(j) == quad, one, zero))
            tiles.append([jnp.concatenate(rows, axis=0), hot])
    return tiles


def grids_of(total, fields):
    out = []
    for p in range(2 * fields):
        rows = []
        for j in range(QS // 8):
            at = (j * 2 * fields + p) * 16
            rows.append(total[at : at + 8] + total[at + 8 : at + 16])
        out.append(jnp.concatenate(rows, axis=0))
    at = QS // 8 * 2 * fields * 16
    return total[at : at + QS], out[0::2], out[1::2]


def kernel(
    nrows,
    nchan,
    rad_in,
    band_in,
    rib_in,
    col_in,
    cnt_out,
    mean_out,
    var_out,
    spr_out,
    dep_out,
    rad_ref,
    band_ref,
    rib_ref,
    col_ref,
    staged,
    sent,
    arrived,
    col_hot,
    part_s,
    part_r,
    pairs,
    back_s,
    back_r,
    scale_r,
    turned,
    ledger,
    ready,
    ins,
    send,
    came,
    back,
    scales,
    shares,
):
    me = lax.axis_index("rows")
    mc = lax.axis_index("chan")
    fields, obs = rad_ref.shape
    cap = 2 * obs // nrows
    lines = cap // LANES
    npair = nchan // 2
    half_rows = nrows // 2
    far = sorted(range(1, nrows), key=lambda d: (d // half_rows, d % 2, d), reverse=True)
    row_peer = [flip(me, d) for d in range(nrows)]
    chan_peer = [lax.rem(mc + 2 * j, nchan) for j in range(npair)]
    partner = flip(mc, 1)

    def wait_all(ref, semaphore):
        pltpu.make_async_copy(ref, ref, semaphore).wait()

    def remote(src, dst, recv, kind=0, **to):
        return pltpu.make_async_remote_copy(
            src_ref=src,
            dst_ref=dst,
            send_sem=send.at[kind],
            recv_sem=recv,
            device_id=to,
            device_id_type=MESH,
        )

    barrier = pltpu.get_barrier_semaphore()
    for d in far:
        pl.semaphore_signal(
            barrier, inc=1, device_id={"rows": row_peer[d]}, device_id_type=MESH
        )
    for e in range(1, nchan):
        pl.semaphore_signal(barrier, inc=1, device_id={"chan": flip(mc, e)}, device_id_type=MESH)
    fetches = [
        pltpu.make_async_copy(a, b, ins.at[min(i, 1)])
        for i, (a, b) in enumerate(
            ((band_in, band_ref), (rad_in, rad_ref), (rib_in, rib_ref), (col_in, col_ref))
        )
    ]
    for fetch in fetches:
        fetch.start()

    fetches[0].wait()
    dest = band_ref[...]

    def place_all(acc_rank, *accs):
        ranks = rank_of(dest, nrows, acc_rank)
        rank = folded(jnp.concatenate(ranks, axis=1)).astype(jnp.int32)
        wide = min(cap, LOW)
        parts = cap // wide
        hots, keys = [], []
        for k in range(obs // LANES):
            upper = jnp.floor(ranks[k] * (1.0 / wide))
            hots.append(low_hot(ranks[k] - upper * wide, LOW))
            names = jnp.bitwise_xor(dest[:, k * LANES : (k + 1) * LANES], me)
            keys.append(packed(names.astype(F32) * parts + upper))
        wait_all(staged.at[: (fields + 2) * obs // LANES], ins.at[1])
        high, rest = two(rad_ref[...])
        middle, low = two(rest)
        col = col_ref[...]
        code = (col // LOW) * ROWS_DEV + rib_ref[...] + 1
        payload = jnp.concatenate(
            [high, middle, low]
            + [code.astype(F32), (col & (LOW - 1)).astype(F32)]
            + [jnp.zeros((PACK - 3 * fields - 2, obs), F32)],
            axis=0,
        ).astype(BF16)
        zero = jnp.zeros((PACK, LANES), BF16)
        left = []
        for k in range(obs // LANES):
            load = payload[:, k * LANES : (k + 1) * LANES]
            left.append(
                jnp.concatenate(
                    [
                        jnp.where(keys[k] == jnp.full((PACK, LANES), key, BF16), load, zero)
                        for key in range(nrows * parts)
                    ],
                    axis=0,
                )
            )
        product(accs, [list(x) for x in zip(left, hots)], True)
        placed = pltpu.matmul_pop(accs[0]) + pltpu.matmul_pop(accs[1])
        for d in far + [0]:
            target = sent if d > 0 else arrived
            for p in range(parts):
                part = placed[(d * parts + p) * PACK : (d * parts + p + 1) * PACK]
                values = (part[:fields] + part[fields : 2 * fields]) + part[2 * fields : 3 * fields]
                cells = part[3 * fields : 3 * fields + 1] * LOW + part[3 * fields + 1 : 3 * fields + 2]
                for i in range(wide // LANES):
                    t = p * (wide // LANES) + i
                    span = slice(i * LANES, (i + 1) * LANES)
                    at = (d * lines + t) * 8
                    staged[at : at + fields] = values[:, span]
                    staged[at + fields : at + fields + 1] = cells[:, span]
            for f in range(fields + 1):
                target[d, f] = staged[pl.ds(d * lines * 8 + f, lines, stride=8), :]
        return rank

    rows_placed = nrows * max(1, cap // LOW) * PACK
    rank = pl.run_scoped(
        place_all,
        pltpu.ACC(0)((nrows * obs // LOW, LOW), F32),
        pltpu.ACC(0)((rows_placed, LOW), F32),
        pltpu.ACC(1)((rows_placed, LOW), F32),
    )
    pl.semaphore_wait(barrier, nrows + nchan - 2)
    for d in far:
        remote(
            sent.at[d], arrived.at[d], came.at[d // half_rows + (d + 1) // nrows], rows=row_peer[d]
        ).start()
    for e in range(1, nchan):
        pl.semaphore_signal(ready, inc=1, device_id={"chan": flip(mc, e)}, device_id_type=MESH)


    def cells_all(acc_0, acc_1, *looks):
        accs = (acc_0, acc_1)
        groups = [[0], list(range(1, half_rows)), list(range(half_rows, nrows - 1)), [nrows - 1]]
        for slots in groups:
            if slots[0] == nrows - 1:
                wait_all(sent.at[1:], send.at[0])
                pl.semaphore_wait(ready, nchan - 1)
            if slots[0] > 0:
                at = slots[0] // half_rows + (slots[0] + 1) // nrows
                wait_all(arrived.at[slots[0] : slots[-1] + 1], came.at[at])
            product(accs, tiles_of(arrived, col_hot, slots), True)

        total = pltpu.matmul_pop(accs[0]) + pltpu.matmul_pop(accs[1])
        count, firsts, seconds = grids_of(total, fields)
        inverse = 1.0 / jnp.maximum(count, 1.0)
        partial = None
        means, variances = [], []
        for f in range(fields):
            mean = firsts[f] * inverse
            variance = jnp.maximum(seconds[f] * inverse - mean * mean, 0.0)
            means.append(mean)
            variances.append(variance)
            partial = variance if partial is None else partial + variance

        split = [two(x) for x in means + [partial]]
        pad = jnp.zeros((-(fields + 1) * QS % PACK, LOW), F32)
        table = [jnp.concatenate([x[k] for x in split] + [pad], axis=0).astype(BF16) for k in (0, 1)]
        places = [(d, t) for d in far + [0] for t in range(lines)]
        tiles = [places[i : i + 2] for i in range(0, len(places), 2)]

        def issue(i):
            register = i // 2 % 2
            hot = jnp.concatenate(
                [col_hot[d, :, t * LANES : (t + 1) * LANES] for d, t in tiles[i]], axis=1
            )
            acc = looks[i % len(looks)]
            pltpu.matmul_push_rhs(hot, staging_register=register, mxu_index=i % 2)
            pltpu.matmul_acc_lhs(acc, table[0], load_staged_rhs=register)
            pltpu.matmul_acc_lhs(acc, table[1])

        for i in range(min(len(looks), len(tiles))):
            issue(i)
        for i, tile in enumerate(tiles):
            picked = pltpu.matmul_pop(looks[i % len(looks)])
            if i + len(looks) < len(tiles):
                issue(i + len(looks))
            for k, (d, t) in enumerate(tile):
                span = slice(k * LANES, (k + 1) * LANES)
                target = back_s if d > 0 else back_r
                high = arrived[d, fields, t : t + 1].astype(jnp.int32) // LOW - 1
                here = iota((QS, LANES), 0) == high
                for f in range(fields + 1):
                    both = picked[f * QS : (f + 1) * QS, span]
                    found = jnp.sum(jnp.where(here, both, 0.0), axis=0, keepdims=True)
                    if f < fields:
                        target[d, f, t : t + 1] = arrived[d, f, t : t + 1] - found
                    else:
                        target[d, f, t : t + 1] = found
                if t < lines - 1:
                    continue
                for e in range(nchan - 1, 0, -1):
                    slot = e * nrows + d
                    remote(
                        target.at[d, fields],
                        scale_r.at[slot],
                        scales.at[d // half_rows],
                        rows=row_peer[d],
                        chan=flip(mc, e),
                    ).start()
                if d > 0:
                    remote(
                        back_s.at[d], back_r.at[d], back.at[d // half_rows], rows=row_peer[d]
                    ).start()
        part_s[...] = partial
        part_copy = remote(part_s, part_r, shares.at[0], 1, chan=partner)
        part_copy.start()

        spill(cnt_out, count)
        for f in range(fields):
            spill(mean_out.at[f], means[f])
            spill(var_out.at[f], variances[f])
        part_copy.wait_recv()
        mine = mc // 2
        pairs[mine] = part_s[...] + part_r[...]
        for j in range(1, npair):
            remote(pairs.at[mine], pairs.at[mine], shares.at[1], 1, chan=chan_peer[j]).start()

        place = jnp.bitwise_xor(folded(dest), me) * lines + rank // LANES
        lane = rank & (LANES - 1)
        found = [jnp.zeros(rank.shape, F32) for _ in range(fields + 1)]
        far_half = list(range(nrows - 1, half_rows - 1, -1))
        returns = [list(range(half_rows)), far_half]
        for slots in returns:
            first = max(1, min(slots))
            wait_all(back_r.at[first : max(slots) + 1], back.at[first // half_rows])
            for d in slots:
                for t in range(lines):
                    here = place == d * lines + t
                    for f in range(fields):
                        found[f] = jnp.where(here, take(back_r[d, f, t : t + 1], lane), found[f])
        wait_all(pairs.at[1:], shares.at[1])
        spread = pairs[0]
        for p in range(1, npair):
            spread = spread + pairs[p]
        spill(spr_out, spread)
        lent = (nrows - 1) * (fields + 1) + (nchan - 1) * nrows
        wait_all(ledger.at[:lent], send.at[0])
        wait_all(pairs, send.at[1])
        for slots in returns:
            wait_all(
                scale_r.at[nrows : nrows + (nchan - 1) * len(slots)],
                scales.at[slots[0] // half_rows],
            )
            for d in slots:
                for t in range(lines):
                    here = place == d * lines + t
                    row = back_r[d, fields, t : t + 1]
                    for e in range(1, nchan):
                        row = row + scale_r[e * nrows + d, t : t + 1]
                    found[fields] = jnp.where(here, take(row, lane), found[fields])
        scale = lax.rsqrt(1.0 + found[fields] / CHAN)
        many = obs // LANES
        for f in range(fields):
            turned[f * many : (f + 1) * many] = found[f] * scale
        for k in range(many):
            dep_out[:, k * LANES : (k + 1) * LANES] = turned[pl.ds(k, fields, stride=many), :]

    rows_summed = QS * 4 * fields + -(-QS // PACK) * PACK
    rows_looked = -(-(fields + 1) * QS // PACK) * PACK
    pl.run_scoped(
        cells_all,
        *(pltpu.ACC(unit)((rows_summed, LOW), F32) for unit in (0, 1)),
        *(pltpu.ACC(unit)((rows_looked, LOW), F32) for unit in (0, 1) * 4),
    )


def finish(*refs):
    half = len(refs) // 2

    def store(sems):
        copies = [
            pltpu.make_async_copy(a, b, sems.at[i])
            for i, (a, b) in enumerate(zip(refs[:half], refs[half:]))
        ]
        for copy in copies:
            copy.start()
        for copy in copies:
            copy.wait()

    pl.run_scoped(store, pltpu.SemaphoreType.DMA((half,)))


def body(radiances, band, row_in_band, column):
    nrows = lax.axis_size("rows")
    nchan = lax.axis_size("chan")
    fields, obs = radiances.shape
    cap = 2 * obs // nrows
    lines = cap // LANES
    npair = nchan // 2
    vmem = pl.BlockSpec(memory_space=pltpu.VMEM)
    anywhere = pl.BlockSpec(memory_space=pl.ANY)
    dma = pltpu.SemaphoreType.DMA
    shapes = (
        ((ROWS_DEV, COLS), jnp.int32),
        ((fields, ROWS_DEV, COLS), F32),
        ((fields, ROWS_DEV, COLS), F32),
        ((ROWS_DEV, COLS), F32),
        ((fields, obs), F32),
    )
    held = pl.pallas_call(
        functools.partial(kernel, nrows, nchan),
        out_shape=tuple(pltpu.VMEM(s, t) for s, t in shapes),
        in_specs=[pl.BlockSpec(memory_space=pltpu.HBM)] * 4,
        out_specs=(vmem,) * len(shapes),
        scratch_shapes=[
            pltpu.VMEM((fields, obs), F32),
            pltpu.VMEM((1, obs), jnp.int32),
            pltpu.VMEM((1, obs), jnp.int32),
            pltpu.VMEM((1, obs), jnp.int32),
            pltpu.VMEM((nrows * lines * 8, LANES), F32),
            pltpu.VMEM((nrows, fields + 1, lines, LANES), F32),
            pltpu.VMEM((nrows, fields + 1, lines, LANES), F32),
            pltpu.VMEM((nrows, LOW, cap), BF16),
            pltpu.VMEM((QS, LOW), F32),
            pltpu.VMEM((QS, LOW), F32),
            pltpu.VMEM((npair, QS, LOW), F32),
            pltpu.VMEM((nrows, fields + 1, lines, LANES), F32),
            pltpu.VMEM((nrows, fields + 1, lines, LANES), F32),
            pltpu.VMEM((nchan * nrows, lines, LANES), F32),
            pltpu.VMEM((fields * obs // LANES, LANES), F32),
            pltpu.VMEM((nrows * (fields + nchan), lines, LANES), F32),
            pltpu.SemaphoreType.REGULAR,
            dma((2,)),
            dma((2,)),
            dma((3,)),
            dma((2,)),
            dma((2,)),
            dma((2,)),
        ],
        compiler_params=pltpu.CompilerParams(
            collective_id=0, has_side_effects=True, vmem_limit_bytes=32 * 1024 * 1024
        ),
    )(
        *(
            pltpu.with_memory_space_constraint(x, pltpu.HBM)
            for x in (
                radiances,
                band.reshape(1, obs),
                row_in_band.reshape(1, obs),
                column.reshape(1, obs),
            )
        )
    )
    return pl.pallas_call(
        finish,
        out_shape=tuple(jax.ShapeDtypeStruct(s, t) for s, t in shapes),
        in_specs=[vmem] * len(shapes),
        out_specs=(anywhere,) * len(shapes),
        compiler_params=pltpu.CompilerParams(vmem_limit_bytes=32 * 1024 * 1024),
    )(*held)


def solution(mesh):
    in_specs = (P("chan", "rows"), P("rows", None), P("rows"), P("rows"))
    out_specs = (
        P("rows", None),
        P("chan", "rows", None),
        P("chan", "rows", None),
        P("rows", None),
        P("chan", "rows"),
    )
    return jax.shard_map(body, mesh=mesh, in_specs=in_specs, out_specs=out_specs, check_vma=False)
```
